768 devices in a mesh: band: 192 (over y, z, core), ga: 4 (over x).
Axes of the slice: x: 4, y: 8, z: 12, core: 2. Of those that a mesh axis runs over, the one named last changes fastest.
Arguments:
- orbitals: bfloat16 [2, 192, 160, 128], P(None, 'band', 'ga'), may hold values from -8 to 8, as said below
- potential: float32 [480, 480], P('ga'), may hold values from -2 to 2
- slot_sticks: int32 [160], replicated, may hold values from -1 to 126, as said below
- stick_entries: int32 [160, 128], replicated, may hold values from -1 to 126, as said below
Outputs:
- applied_orbitals: bfloat16 [2, 192, 160, 128], P(None, 'band', 'ga')
- correlation: float32 [2, 192, 192], replicated
- reduced_hamiltonian: float32 [2, 192, 192], replicated
The draws below stay inside these ranges and needn't reach their ends.
Inputs may be any that keep to these rules, and one draw needn't show every extreme that they name: `slot_sticks`: every gx with |gx| < 64 is held by exactly one slot; the other slots hold -1. Slots t with t // 40 = d are those of index d of ga; on some index of ga all 40 slots hold sticks. `stick_entries`: row t lists, in some order, gz + 63 for every gz with gx^2 + gz^2 < 64^2, gx being the stick of slot t, then -1 to the end of the row; rows of empty slots are all -1. `orbitals`: entries where stick_entries is -1 carry values that are not used.
All inputs are finite; a program needn't handle non-finite values.
Results may differ from the reference program's by a relative error of at most 0.001.
Values may be sent and summed in bfloat16 or wider, within the bound.
No kernel may reach another device: no remote copies, remote signals or barrier semaphores. Data moves between devices by JAX's collectives and lax.ppermute only.
A program may use at most 32 MiB of HBM per device.

```python
import jax
import jax.numpy as jnp
from jax import lax

NGRID = 480
RAD = 64
KMAX = 128
SLOTS = 40
SLOT_ALL = 160
NB = 192
N_GA = 4


def stick_layout(key):
    stick_count = 2 * RAD - 1
    key_device, key_picked, key_ordering = jax.random.split(jax.random.fold_in(key, 11), 3)
    full_device = jax.random.randint(key_device, (), 0, N_GA)
    slot_ids = jnp.arange(SLOT_ALL, dtype=jnp.int32)
    owners = slot_ids // SLOTS
    others = jnp.where(owners > full_device, slot_ids - SLOTS, slot_ids)
    picked = jax.random.permutation(key_picked, (N_GA - 1) * SLOTS).astype(jnp.int32)
    chosen = jnp.take(picked, jnp.clip(others, 0, (N_GA - 1) * SLOTS - 1)) < stick_count - SLOTS
    occupied = jnp.where(owners == full_device, True, chosen)
    ranking = jnp.cumsum(occupied.astype(jnp.int32)) - 1
    ordering = jax.random.permutation(key_ordering, stick_count).astype(jnp.int32)
    return jnp.where(occupied, jnp.take(ordering, jnp.clip(ranking, 0, stick_count - 1)), -1).astype(jnp.int32)


def draw_slot_sticks(key, part):
    return stick_layout(key)


def draw_stick_entries(key, part):
    sticks = stick_layout(key)
    gx_value = sticks - RAD + 1
    offsets = jnp.arange(RAD, dtype=jnp.int32)
    half_width = jnp.sum((offsets * offsets)[None, :] + (gx_value * gx_value)[:, None] < RAD * RAD, axis=1).astype(jnp.int32) - 1
    length = jnp.where(sticks >= 0, 2 * half_width + 1, 0)
    column_ids = jnp.arange(KMAX, dtype=jnp.int32)
    inside = column_ids[None, :] < length[:, None]
    positions = jnp.where(inside, RAD - 1 - half_width[:, None] + column_ids[None, :], -1)
    jitter = jax.random.randint(jax.random.fold_in(key, 23), (SLOT_ALL, KMAX), 0, 4096)
    scores = jnp.where(inside, jitter, 4096) * KMAX + column_ids[None, :]
    ordering = jnp.argsort(scores, axis=1)
    return jnp.take_along_axis(positions, ordering, axis=1).astype(jnp.int32)


def draw_orbitals(key, part):
    key_own, key_common, key_weight, key_flip = jax.random.split(jax.random.fold_in(key, 37), 4)
    private = jax.random.normal(key_own, (2, NB, SLOT_ALL, KMAX), jnp.float32)
    weight = jax.random.uniform(key_weight, (NB,), jnp.float32, 0.5, 1.5)
    common = jax.random.normal(key_common, (2, 1, SLOT_ALL, KMAX), jnp.float32)
    sign_flip = jnp.where(jax.random.bernoulli(key_flip, 0.5, (NB,)), 1.0, -1.0)
    values = private + (weight * sign_flip)[None, :, None, None] * common
    return jnp.clip(values, -8.0, 8.0).astype(jnp.bfloat16)


def steps_of(rng, shape, pieces, smallest, high):
    loudness, own = 1.0, jax.random.fold_in(rng, 6)
    for dim, parts in pieces:
        steps = jnp.exp(jax.random.uniform(jax.random.fold_in(own, dim), (parts,), jnp.float32, smallest / len(pieces), high / len(pieces)))
        loudness = loudness * jnp.repeat(steps, shape[dim] // parts).reshape([-1 if axis == dim else 1 for axis in range(len(shape))])
    return loudness


def setup_inputs(seed: int = 0) -> dict:
    key_of = jax.random.split(jax.random.key(seed), 5)
    return {
        "orbitals": draw_orbitals(jax.random.fold_in(key_of[4], 71), 0),
        "potential": jnp.clip(jax.random.uniform(key_of[1], (NGRID, NGRID), jnp.float32, -2.0, 2.0) * steps_of(key_of[1], (NGRID, NGRID), ((0, 4),), -0.4, 0.0), -2.0, 2.0),
        "slot_sticks": draw_slot_sticks(jax.random.fold_in(key_of[4], 71), 0),
        "stick_entries": draw_stick_entries(jax.random.fold_in(key_of[4], 71), 0),
    }


TWO_PI = 6.283185307179586
HIGHEST_PRECISION = lax.Precision.HIGHEST


def phases(frequency, position, points):
    winding = (frequency[:, None] * position[None, :]) % points
    angles = winding.astype(jnp.float32) * (TWO_PI / points)
    return jnp.cos(angles), jnp.sin(angles)


def stick_phases(slot_sticks, radius, points):
    frequency = slot_sticks - radius + 1
    x_cos, x_sin = phases(frequency, jnp.arange(points, dtype=jnp.int32), points)
    filled = (slot_sticks >= 0).astype(jnp.float32)[:, None]
    return x_cos * filled, x_sin * filled


def unpack(coeffs, entry_lists):
    slot_count, width = entry_lists.shape
    leading = coeffs.shape[:2]
    flat_index = jnp.where(entry_lists >= 0, entry_lists + width * jnp.arange(slot_count, dtype=jnp.int32)[:, None], slot_count * width)
    spread = jnp.zeros(leading + (slot_count * width,), jnp.float32)
    values = coeffs.reshape(leading + (slot_count * width,)).astype(jnp.float32)
    spread = spread.at[:, :, flat_index.reshape(-1)].add(values, mode="drop")
    return spread.reshape(coeffs.shape)


def z_forward(spread, z_cos, z_sin):
    real_part = jnp.einsum("bsp,pz->bsz", spread[0], z_cos, precision=HIGHEST_PRECISION) - jnp.einsum("bsp,pz->bsz", spread[1], z_sin, precision=HIGHEST_PRECISION)
    imag_part = jnp.einsum("bsp,pz->bsz", spread[0], z_sin, precision=HIGHEST_PRECISION) + jnp.einsum("bsp,pz->bsz", spread[1], z_cos, precision=HIGHEST_PRECISION)
    return jnp.stack([real_part, imag_part])


def plane_work(columns, x_cos, x_sin, potential):
    field_real = jnp.einsum("bsz,sx->bzx", columns[0], x_cos, precision=HIGHEST_PRECISION) - jnp.einsum("bsz,sx->bzx", columns[1], x_sin, precision=HIGHEST_PRECISION)
    field_imag = jnp.einsum("bsz,sx->bzx", columns[0], x_sin, precision=HIGHEST_PRECISION) + jnp.einsum("bsz,sx->bzx", columns[1], x_cos, precision=HIGHEST_PRECISION)
    prod_real = potential[None] * field_real
    prod_imag = potential[None] * field_imag
    back_real = jnp.einsum("bzx,sx->bsz", prod_real, x_cos, precision=HIGHEST_PRECISION) + jnp.einsum("bzx,sx->bsz", prod_imag, x_sin, precision=HIGHEST_PRECISION)
    back_imag = jnp.einsum("bzx,sx->bsz", prod_imag, x_cos, precision=HIGHEST_PRECISION) - jnp.einsum("bzx,sx->bsz", prod_real, x_sin, precision=HIGHEST_PRECISION)
    return jnp.stack([back_real, back_imag])


def z_backward(gathered, z_cos, z_sin, points):
    real_part = jnp.einsum("bsz,pz->bsp", gathered[0], z_cos, precision=HIGHEST_PRECISION) + jnp.einsum("bsz,pz->bsp", gathered[1], z_sin, precision=HIGHEST_PRECISION)
    imag_part = jnp.einsum("bsz,pz->bsp", gathered[1], z_cos, precision=HIGHEST_PRECISION) - jnp.einsum("bsz,pz->bsp", gathered[0], z_sin, precision=HIGHEST_PRECISION)
    return jnp.stack([real_part, imag_part]) / float(points * points)


def kinetic_factor(sticks, entry_lists, radius):
    gx_value = sticks - radius + 1
    gz_value = entry_lists - radius + 1
    return ((gx_value * gx_value)[:, None] + gz_value * gz_value).astype(jnp.float32) / float(radius * radius)


def cross_products(left, right, scale):
    dims = (((1,), (1,)), ((), ()))
    real_part = lax.dot_general(left[0], right[0], dims, preferred_element_type=jnp.float32) + lax.dot_general(left[1], right[1], dims, preferred_element_type=jnp.float32)
    imag_part = lax.dot_general(left[0], right[1], dims, preferred_element_type=jnp.float32) - lax.dot_general(left[1], right[0], dims, preferred_element_type=jnp.float32)
    return jnp.stack([real_part, imag_part]) * scale


def reference(orbitals, potential, slot_sticks, stick_entries):
    points = potential.shape[1]
    width = stick_entries.shape[1]
    radius = width // 2
    band_total = orbitals.shape[1]
    present = stick_entries >= 0
    masked = jnp.where(present[None, None], orbitals, jnp.zeros_like(orbitals))
    spread = unpack(orbitals, stick_entries)
    frequency = jnp.arange(width, dtype=jnp.int32) - radius + 1
    z_cos, z_sin = phases(frequency, jnp.arange(points, dtype=jnp.int32), points)
    x_cos, x_sin = stick_phases(slot_sticks, radius, points)

    def one_band(coeffs):
        columns = z_forward(coeffs[:, None], z_cos, z_sin)
        gathered = plane_work(columns, x_cos, x_sin, potential)
        return z_backward(gathered, z_cos, z_sin, points)[:, 0]

    spectra = jnp.moveaxis(lax.map(one_band, jnp.moveaxis(spread, 1, 0)), 0, 1)
    indices = jnp.broadcast_to(jnp.clip(stick_entries, 0, width - 1)[None, None], spectra.shape)
    applied = jnp.take_along_axis(spectra, indices, axis=3)
    kinetic = kinetic_factor(slot_sticks, stick_entries, radius)
    applied_orbitals = jnp.where(present[None, None], kinetic[None, None] * orbitals.astype(jnp.float32) + applied, jnp.float32(0.0)).astype(jnp.bfloat16)
    scale = 1.0 / (4.0 * radius * radius)
    flat_psi = masked.reshape(2, band_total, -1)
    flat_h = applied_orbitals.reshape(2, band_total, -1)
    correlation = cross_products(flat_psi, flat_psi, scale)
    reduced_hamiltonian = cross_products(flat_psi, flat_h, scale)
    return applied_orbitals, correlation, reduced_hamiltonian
```

```python
import functools

import jax
import jax.numpy as jnp
import numpy as np
from jax import lax
from jax.experimental import pallas as pl
from jax.experimental.pallas import tpu as pltpu
from jax.sharding import Mesh
from jax.sharding import PartitionSpec as P

BAND = ("y", "z", "c")
M = 256
F32 = jnp.float32
BF16 = jnp.bfloat16


def hi_lo(table):
    hi = table.astype(np.float32).astype(jnp.bfloat16)
    lo = (table - hi.astype(np.float64)).astype(np.float32).astype(jnp.bfloat16)
    return np.stack([hi, lo])


def tables(points, radius):
    freq = np.arange(2 * radius) - radius + 1
    pos = np.arange(M)
    ang = 2.0 * np.pi * ((freq[:, None] * pos[None, :]) % M) / M
    cos, sin = np.cos(ang), np.sin(ang)
    wz = np.block([[cos, sin], [-sin, cos]])
    top = 2 * radius - 2
    q = np.arange(1, top + 1)
    shift = pos[:, None] / M - np.arange(points)[None, :] / points
    resample = np.ones((M, points))
    for k in q:
        resample += 2.0 * np.cos(2.0 * np.pi * k * shift)
    resample /= points
    return hi_lo(wz), hi_lo(wz.T), hi_lo(resample.T), hi_lo(resample)


def split(x):
    hi = x.astype(BF16)
    return hi, (x - hi.astype(F32)).astype(BF16)


def mm(a, b):
    return lax.dot_general(a, b, (((1,), (0,)), ((), ())), preferred_element_type=F32)


def mm_nt(a, b):
    return lax.dot_general(a, b, (((1,), (1,)), ((), ())), preferred_element_type=F32)


def first_kernel(ent_ref, orb_ref, pot_ref, bx_ref, packed_ref, own_ref):
    ent_t = ent_ref[...].T
    lane = lax.broadcasted_iota(jnp.int32, (128, 128), 1)
    sub = lax.broadcasted_iota(jnp.int32, (128, 128), 0)
    pieces = [[], []]
    for g in range(8):
        rows = []
        for r in range(5):
            s = 8 * g + r
            match = ent_t[:, s : s + 1] == lane
            rows.append(jnp.max(jnp.where(match, sub, -1), axis=0, keepdims=True))
        rows.append(jnp.full((3, 128), -1, jnp.int32))
        source = jnp.concatenate(rows, axis=0)
        index = jnp.maximum(source, 0)
        for c in range(2):
            block = orb_ref[c, 8 * g : 8 * g + 8, :]
            moved = jnp.take_along_axis(block, index, axis=1)
            pieces[c].append(jnp.where(source >= 0, moved, 0.0))
    spread = jnp.concatenate(pieces[0] + pieces[1], axis=0).astype(BF16)
    own_ref[...] = spread
    packed_ref[0:128, :] = spread
    v_hi, v_lo = split(pot_ref[...])
    vx = mm(v_hi, bx_ref[0]) + mm(v_lo, bx_ref[0]) + mm(v_hi, bx_ref[1])
    vx = jnp.concatenate([vx[:, :128], vx[:, 128:]], axis=0)
    hi, lo = split(vx)
    packed_ref[128:368, :] = hi
    packed_ref[368:608, :] = lo


def main_kernel(all_ref, own_ref, ent_ref, slot_row_ref, slot_col_ref, wz_ref, wx_ref, bz_ref, msg_ref, out_ref):
    def gathered_v(first):
        left = jnp.concatenate([all_ref[d, first : first + 120, :].astype(F32) for d in range(4)], axis=0)
        right = jnp.concatenate([all_ref[d, first + 120 : first + 240, :].astype(F32) for d in range(4)], axis=0)
        return jnp.concatenate([left, right], axis=1).astype(BF16)

    v_hi = gathered_v(128)
    v_lo = gathered_v(368)
    pot = mm(bz_ref[0], v_hi) + mm(bz_ref[1], v_hi) + mm(bz_ref[0], v_lo)
    pot = pot.T

    place = (
        lax.broadcasted_iota(jnp.int32, (128, 256), 0) == jnp.broadcast_to(slot_row_ref[...], (128, 256))
    ).astype(F32).astype(BF16)
    c_re = jnp.concatenate([all_ref[d, 0:64, :] for d in range(4)], axis=0)
    c_im = jnp.concatenate([all_ref[d, 64:128, :] for d in range(4)], axis=0)
    sticks = jnp.concatenate([mm(place, c_re), mm(place, c_im)], axis=0).astype(BF16)

    t = mm(wx_ref[0], sticks) + mm(wx_ref[1], sticks)
    t = jnp.concatenate([t[:M], t[M:]], axis=1)
    t_hi, t_lo = split(t)
    field = mm(t_hi, wz_ref[0]) + mm(t_lo, wz_ref[0]) + mm(t_hi, wz_ref[1])
    prod = jnp.concatenate([field[:, :M] * pot, field[:, M:] * pot], axis=1)
    p_hi, p_lo = split(prod)
    y = mm(p_hi, wx_ref[0]) + mm(p_lo, wx_ref[0]) + mm(p_hi, wx_ref[1])
    y = jnp.concatenate([y[:, :128], y[:, 128:]], axis=0)
    y_hi, y_lo = split(y)

    slot = slot_col_ref[...]
    pick = (lax.broadcasted_iota(jnp.int32, (64, 128), 1) == slot).astype(F32).astype(BF16)
    none = jnp.zeros((64, 128), BF16)
    pick = jnp.concatenate(
        [jnp.concatenate([pick, none], axis=1), jnp.concatenate([none, pick], axis=1)], axis=0
    )
    w_hi = mm(pick, wz_ref[0]).astype(BF16)
    w_lo = mm(pick, wz_ref[1]).astype(BF16)
    applied = (mm(w_hi, y_hi) + mm(w_hi, y_lo) + mm(w_lo, y_hi)) * (1.0 / (M * M))

    gx = slot - 63
    gz = lax.broadcasted_iota(jnp.int32, (64, 128), 1) - 63
    square = gx * gx + gz * gz
    inside = (square < 64 * 64) & (slot >= 0)
    kinetic = square.astype(F32) * (1.0 / 4096.0)
    own = own_ref[...].astype(F32)
    h = []
    for c in range(2):
        value = kinetic * own[64 * c : 64 * c + 64] + applied[64 * c : 64 * c + 64]
        h.append(jnp.where(inside, value, 0.0).astype(BF16).astype(F32))
    ent = ent_ref[...]
    index = jnp.maximum(ent, 0)
    for c in range(2):
        for g in range(8):
            rows = slice(8 * g, 8 * g + 8)
            moved = jnp.take_along_axis(h[c][rows], index[rows], axis=1)
            out_ref[c, rows, :] = jnp.where(ent[rows] >= 0, moved, 0.0)
    for g in range(8):
        rows = slice(8 * g, 8 * g + 8)
        msg = [own[rows], own[64 + 8 * g : 72 + 8 * g], h[0][rows], h[1][rows]]
        msg_ref[g] = jnp.concatenate(msg, axis=0).astype(BF16)


def product_kernel(psi_ref, own_ref, block_ref, psi_s, own_s):
    for c in range(2):
        for z in range(12):
            for y in range(8):
                band = y * 24 + z * 2 + c
                psi_s[16 * band : 16 * band + 16, :] = psi_ref[c, z, y].astype(F32)
    for y in range(8):
        own_s[32 * y : 32 * y + 32, :] = own_ref[y].astype(F32)

    def entries(ref, part, count, pitch):
        rows = [ref[pl.ds(8 * part + r, count, stride=pitch), :] for r in range(5)]
        return jnp.concatenate(rows, axis=1)

    p_re = entries(psi_s, 0, 192, 16).astype(BF16)
    p_im = entries(psi_s, 1, 192, 16).astype(BF16)
    m_re, m_im, a_re, a_im = [entries(own_s, q, 8, 32) for q in range(4)]
    left_re = jnp.concatenate([m_re, m_im, a_re, a_im], axis=0).astype(BF16)
    left_im = jnp.concatenate([m_im, -m_re, a_im, -a_re], axis=0).astype(BF16)
    block = (mm_nt(left_re, p_re) + mm_nt(left_im, p_im)) * (1.0 / 16384.0)
    block_ref[0:32, :] = block[:, :128]
    block_ref[32:48, :] = jnp.concatenate([block[:16, 128:], block[16:, 128:]], axis=1)


def last_kernel(all_ref, s_ref, h_ref, t_s):
    for c in range(2):
        for z in range(12):
            tail = all_ref[c, z, 32:48, :]
            for m in range(4):
                rows = pl.ds(z * 2 + c, 8, stride=24)
                t_s[2 * m, rows, :] = all_ref[c, z, 8 * m : 8 * m + 8, :]
                half = tail[8 * (m % 2) : 8 * (m % 2) + 8]
                if m >= 2:
                    half = jnp.concatenate([half[:, 64:], half[:, :64]], axis=1)
                t_s[2 * m + 1, rows, :] = half
    for m in range(4):
        ref = s_ref if m < 2 else h_ref
        ref[m % 2, 0:128, :] = t_s[2 * m].T
        ref[m % 2, 128:192, :] = t_s[2 * m + 1].T[:64]


def call(kernel, outs, *args, scratch=()):
    return pl.pallas_call(
        kernel,
        out_shape=outs,
        scratch_shapes=list(scratch),
        compiler_params=pltpu.CompilerParams(vmem_limit_bytes=48 * 1024 * 1024),
    )(*args)


def shape(dims, dtype):
    return jax.ShapeDtypeStruct(dims, dtype)


def body(orbitals, potential, slot_sticks, stick_entries):
    points = potential.shape[1]
    wz, wx, bx, bz = tables(points, 64)
    ga = lax.axis_index("x")
    own_lists = lax.dynamic_slice_in_dim(stick_entries, ga * 40, 40, 0)
    ent = jnp.pad(own_lists.reshape(8, 5, 128), ((0, 0), (0, 3), (0, 0)), constant_values=-1).reshape(64, 128)
    slots = jnp.pad(slot_sticks.reshape(32, 5), ((0, 0), (0, 3)), constant_values=-1)
    slot_row = slots.reshape(1, 256)
    slot_col = lax.dynamic_slice_in_dim(slots, ga * 8, 8, 0).reshape(64, 1)
    orb = jnp.pad(
        orbitals.reshape(2, 8, 5, 128).astype(F32), ((0, 0), (0, 0), (0, 3), (0, 0))
    ).reshape(2, 64, 128)
    packed, own = call(
        first_kernel, [shape((608, 128), BF16), shape((128, 128), BF16)], ent, orb, potential, bx
    )
    everyone = lax.all_gather(packed, "x")
    msg, out = call(
        main_kernel,
        [shape((8, 32, 128), BF16), shape((2, 64, 128), F32)],
        everyone, own, ent, slot_row, slot_col, wz, wx, bz,
    )
    applied_orbitals = out.reshape(2, 8, 8, 128)[:, :, :5].reshape(2, 1, 40, 128).astype(BF16)
    arrived = lax.all_to_all(msg, "y", 0, 0, tiled=True)
    psi = lax.all_gather(arrived[:, :16], "z")
    psi = lax.all_gather(psi, "c")
    block = call(
        product_kernel,
        shape((48, 128), F32),
        psi, arrived,
        scratch=[pltpu.VMEM((192 * 16, 128), F32), pltpu.VMEM((8 * 32, 128), F32)],
    )
    block = lax.all_gather(block, "x").sum(axis=0)
    block = lax.all_gather(block, "y").sum(axis=0)
    blocks = lax.all_gather(lax.all_gather(block, "z"), "c")
    correlation, reduced = call(
        last_kernel,
        [shape((2, 192, 192), F32), shape((2, 192, 192), F32)],
        blocks,
        scratch=[pltpu.VMEM((8, 192, 128), F32)],
    )
    return applied_orbitals, correlation, reduced


def solution(mesh):
    finer = Mesh(mesh.devices.reshape(8, 12, 2, mesh.shape["ga"]), ("y", "z", "c", "x"))
    return jax.shard_map(
        body,
        mesh=finer,
        in_specs=(P(None, BAND, "x", None), P("x", None), P(), P()),
        out_specs=(P(None, BAND, "x", None), P(), P()),
        check_vma=False,
    )
```

```python
import functools

import jax
import jax.numpy as jnp
import numpy as np
from jax import lax
from jax.experimental import pallas as pl
from jax.experimental.pallas import tpu as pltpu
from jax.sharding import Mesh
from jax.sharding import PartitionSpec as P

BAND = ("y", "z", "c")
M = 256
F32 = jnp.float32
BF16 = jnp.bfloat16


def hi_lo(table):
    hi = table.astype(np.float32).astype(jnp.bfloat16)
    lo = (table - hi.astype(np.float64)).astype(np.float32).astype(jnp.bfloat16)
    return np.stack([hi, lo])


def tables(points, radius):
    freq = np.arange(2 * radius) - radius + 1
    pos = np.arange(M)
    ang = 2.0 * np.pi * ((freq[:, None] * pos[None, :]) % M) / M
    cos, sin = np.cos(ang), np.sin(ang)
    wz = np.block([[cos, sin], [-sin, cos]])
    top = 2 * radius - 2
    q = np.arange(1, top + 1)
    shift = pos[:, None] / M - np.arange(points)[None, :] / points
    resample = np.ones((M, points))
    for k in q:
        resample += 2.0 * np.cos(2.0 * np.pi * k * shift)
    resample /= points
    return hi_lo(wz), hi_lo(wz.T), hi_lo(resample.T), hi_lo(resample)


def split(x):
    hi = x.astype(BF16)
    return hi, (x - hi.astype(F32)).astype(BF16)


def mm(a, b):
    return lax.dot_general(a, b, (((1,), (0,)), ((), ())), preferred_element_type=F32)


def mm_nt(a, b):
    return lax.dot_general(a, b, (((1,), (1,)), ((), ())), preferred_element_type=F32)


def first_kernel(ent_ref, orb_ref, pot_ref, bx_ref, zmsg_ref, packed_ref, orb_s):
    first = pl.multiple_of(lax.axis_index("x") * 40, 8)
    ent_t = ent_ref[pl.ds(first, 40), :].T
    orb_s[:, 0:40, :] = orb_ref[...].astype(F32)
    orb_s[:, 40:48, :] = jnp.zeros((2, 8, 128), F32)
    lane = lax.broadcasted_iota(jnp.int32, (128, 128), 1)
    sub = lax.broadcasted_iota(jnp.int32, (128, 128), 0)
    pieces = [[], []]
    for g in range(8):
        rows = []
        for r in range(5):
            s = 5 * g + r
            match = ent_t[:, s : s + 1] == lane
            rows.append(jnp.max(jnp.where(match, sub, -1), axis=0, keepdims=True))
        rows.append(jnp.full((3, 128), -1, jnp.int32))
        source = jnp.concatenate(rows, axis=0)
        index = jnp.maximum(source, 0)
        for c in range(2):
            moved = jnp.take_along_axis(orb_s[c, 5 * g : 5 * g + 8, :], index, axis=1)
            pieces[c].append(jnp.where(source >= 0, moved, 0.0))
        group = jnp.concatenate([pieces[0][g], pieces[1][g]], axis=0).astype(BF16)
        for z in range(12):
            zmsg_ref[z, g] = group
    packed_ref[0:128, :] = jnp.concatenate(pieces[0] + pieces[1], axis=0).astype(BF16)
    v_hi, v_lo = split(pot_ref[...])
    vx = mm(v_hi, bx_ref[0]) + mm(v_lo, bx_ref[0]) + mm(v_hi, bx_ref[1])
    vx = jnp.concatenate([vx[:, :128], vx[:, 128:]], axis=0)
    hi, lo = split(vx)
    packed_ref[128:368, :] = hi
    packed_ref[368:608, :] = lo


def main_kernel(
    all_ref, psi_ref, ent_ref, slot_row_ref, slot_col_ref, wz_ref, wx_ref, bz_ref, msg_ref, out_ref, psi_s, ent_s, out_s
):
    d = lax.axis_index("x")

    def gathered_v(first):
        left = jnp.concatenate([all_ref[d, first : first + 120, :].astype(F32) for d in range(4)], axis=0)
        right = jnp.concatenate([all_ref[d, first + 120 : first + 240, :].astype(F32) for d in range(4)], axis=0)
        return jnp.concatenate([left, right], axis=1).astype(BF16)

    v_hi = gathered_v(128)
    v_lo = gathered_v(368)
    pot = mm(bz_ref[0], v_hi) + mm(bz_ref[1], v_hi) + mm(bz_ref[0], v_lo)
    pot = pot.T

    place = (
        lax.broadcasted_iota(jnp.int32, (128, 256), 0) == jnp.broadcast_to(slot_row_ref[...], (128, 256))
    ).astype(F32).astype(BF16)
    c_re = jnp.concatenate([all_ref[d, 0:64, :] for d in range(4)], axis=0)
    c_im = jnp.concatenate([all_ref[d, 64:128, :] for d in range(4)], axis=0)
    sticks = jnp.concatenate([mm(place, c_re), mm(place, c_im)], axis=0).astype(BF16)

    t = mm(wx_ref[0], sticks) + mm(wx_ref[1], sticks)
    t = jnp.concatenate([t[:M], t[M:]], axis=1)
    t_hi, t_lo = split(t)
    field = mm(t_hi, wz_ref[0]) + mm(t_lo, wz_ref[0]) + mm(t_hi, wz_ref[1])
    prod = jnp.concatenate([field[:, :M] * pot, field[:, M:] * pot], axis=1)
    p_hi, p_lo = split(prod)
    y = mm(p_hi, wx_ref[0]) + mm(p_lo, wx_ref[0]) + mm(p_hi, wx_ref[1])
    y = jnp.concatenate([y[:, :128], y[:, 128:]], axis=0)
    y_hi, y_lo = split(y)

    slot = slot_col_ref[...]
    pick = (lax.broadcasted_iota(jnp.int32, (64, 128), 1) == slot).astype(F32).astype(BF16)
    none = jnp.zeros((64, 128), BF16)
    pick = jnp.concatenate(
        [jnp.concatenate([pick, none], axis=1), jnp.concatenate([none, pick], axis=1)], axis=0
    )
    w_hi = mm(pick, wz_ref[0]).astype(BF16)
    w_lo = mm(pick, wz_ref[1]).astype(BF16)
    applied = (mm(w_hi, y_hi) + mm(w_hi, y_lo) + mm(w_lo, y_hi)) * (1.0 / (M * M))

    gx = slot - 63
    gz = lax.broadcasted_iota(jnp.int32, (64, 128), 1) - 63
    square = gx * gx + gz * gz
    inside = (square < 64 * 64) & (slot >= 0)
    kinetic = square.astype(F32) * (1.0 / 4096.0)
    own = all_ref[d, 0:128, :].astype(F32)
    h = []
    for c in range(2):
        value = kinetic * own[64 * c : 64 * c + 64] + applied[64 * c : 64 * c + 64]
        h.append(jnp.where(inside, value, 0.0).astype(BF16).astype(F32))
    ent_s[0:40, :] = ent_ref[pl.ds(pl.multiple_of(d * 40, 8), 40), :]
    ent_s[40:48, :] = jnp.full((8, 128), -1, jnp.int32)
    for g in range(8):
        ent = ent_s[5 * g : 5 * g + 8, :]
        index = jnp.maximum(ent, 0)
        for c in range(2):
            moved = jnp.take_along_axis(h[c][8 * g : 8 * g + 8], index, axis=1)
            out_s[c, 5 * g : 5 * g + 8, :] = jnp.where(ent >= 0, moved, 0.0)
    out_ref[...] = out_s[:, 0:40, :].astype(BF16)

    for z in range(12):
        for g in range(8):
            psi_s[128 * z + 16 * g : 128 * z + 16 * g + 16, :] = psi_ref[z, g].astype(F32)
    for g in range(8):
        rows = []
        for r in range(5):
            for c in range(2):
                rows.append(psi_s[pl.ds(16 * g + 8 * c + r, 12, stride=128), :])
        rows += [h[0][8 * g : 8 * g + 8], h[1][8 * g : 8 * g + 8], jnp.zeros((8, 128), F32)]
        msg_ref[g] = jnp.concatenate(rows, axis=0).astype(BF16)


def product_kernel(both_ref, own_ref, block_ref, all_s, own_s, psi_s):
    for c in range(2):
        for y in range(8):
            at = (8 * c + y) * 144
            all_s[at : at + 144, :] = both_ref[c, y].astype(F32)
            for r in range(5):
                for part in range(2):
                    row = at + 24 * r + 12 * part
                    psi_s[5 * part + r, pl.ds(24 * y + c, 12, stride=2), :] = all_s[row : row + 12, :]
    for y in range(8):
        own_s[144 * y : 144 * y + 144, :] = own_ref[y].astype(F32)
    z = lax.axis_index("z")

    def entries(first, pitch):
        rows = [own_s[pl.ds(first + pitch * r, 8, stride=144), :] for r in range(5)]
        return jnp.concatenate(rows, axis=1)

    m_re, m_im = entries(z, 24), entries(z + 12, 24)
    a_re, a_im = entries(120, 1), entries(128, 1)
    left_re = jnp.concatenate([m_re, m_im, a_re, a_im], axis=0).astype(BF16)
    left_im = jnp.concatenate([m_im, -m_re, a_im, -a_re], axis=0).astype(BF16)
    p_re = jnp.concatenate([psi_s[r] for r in range(5)], axis=1).astype(BF16)
    p_im = jnp.concatenate([psi_s[5 + r] for r in range(5)], axis=1).astype(BF16)
    block = (mm_nt(left_re, p_re) + mm_nt(left_im, p_im)) * (1.0 / 16384.0)
    for x in range(4):
        block_ref[x, 0:32, :] = block[:, :128]
        block_ref[x, 32:48, :] = jnp.concatenate([block[:16, 128:], block[16:, 128:]], axis=1)


def last_kernel(all_ref, s_ref, h_ref, t_s):
    for c in range(2):
        for z in range(12):
            tail = all_ref[c, z, 32:48, :]
            for m in range(4):
                rows = pl.ds(z * 2 + c, 8, stride=24)
                t_s[2 * m, rows, :] = all_ref[c, z, 8 * m : 8 * m + 8, :]
                half = tail[8 * (m % 2) : 8 * (m % 2) + 8]
                if m >= 2:
                    half = jnp.concatenate([half[:, 64:], half[:, :64]], axis=1)
                t_s[2 * m + 1, rows, :] = half
    for m in range(4):
        ref = s_ref if m < 2 else h_ref
        ref[m % 2, 0:128, :] = t_s[2 * m].T
        ref[m % 2, 128:192, :] = t_s[2 * m + 1].T[:64]


def call(kernel, outs, *args, scratch=()):
    return pl.pallas_call(
        kernel,
        out_shape=outs,
        scratch_shapes=list(scratch),
        compiler_params=pltpu.CompilerParams(vmem_limit_bytes=48 * 1024 * 1024),
    )(*args)


def shape(dims, dtype):
    return jax.ShapeDtypeStruct(dims, dtype)


def body(orbitals, potential, slot_sticks, stick_entries):
    wz, wx, bx, bz = tables(potential.shape[1], 64)
    slots = jnp.pad(slot_sticks.reshape(32, 5), ((0, 0), (0, 3)), constant_values=-1)
    slot_row = slots.reshape(1, 256)
    slot_col = lax.dynamic_slice_in_dim(slots, lax.axis_index("x") * 8, 8, 0).reshape(64, 1)
    zmsg, packed = call(
        first_kernel,
        [shape((12, 8, 16, 128), BF16), shape((608, 128), BF16)],
        stick_entries, orbitals.reshape(2, 40, 128), potential, bx,
        scratch=[pltpu.VMEM((2, 48, 128), F32)],
    )
    psi = lax.all_to_all(zmsg, "z", 0, 0, tiled=True)
    everyone = lax.all_gather(packed, "x")
    msg, out = call(
        main_kernel,
        [shape((8, 144, 128), BF16), shape((2, 40, 128), BF16)],
        everyone, psi, stick_entries, slot_row, slot_col, wz, wx, bz,
        scratch=[pltpu.VMEM((1536, 128), F32), pltpu.VMEM((48, 128), jnp.int32), pltpu.VMEM((2, 48, 128), F32)],
    )
    arrived = lax.all_to_all(msg, "y", 0, 0, tiled=True)
    both = lax.all_gather(arrived, "c")
    block = call(
        product_kernel,
        shape((4, 48, 128), F32),
        both, arrived,
        scratch=[pltpu.VMEM((2304, 128), F32), pltpu.VMEM((1152, 128), F32), pltpu.VMEM((10, 192, 128), F32)],
    )
    block = lax.all_to_all(block, "x", 0, 0, tiled=True).sum(axis=0)
    block = lax.all_to_all(jnp.broadcast_to(block, (8, 48, 128)), "y", 0, 0, tiled=True).sum(axis=0)
    block = lax.all_to_all(jnp.broadcast_to(block, (12, 48, 128)), "z", 0, 0, tiled=True)
    correlation, reduced = call(
        last_kernel,
        [shape((2, 192, 192), F32), shape((2, 192, 192), F32)],
        lax.all_gather(block, "c"),
        scratch=[pltpu.VMEM((8, 192, 128), F32)],
    )
    return out.reshape(orbitals.shape), correlation, reduced


def solution(mesh):
    finer = Mesh(mesh.devices.reshape(8, 12, 2, mesh.shape["ga"]), ("y", "z", "c", "x"))
    return jax.shard_map(
        body,
        mesh=finer,
        in_specs=(P(None, BAND, "x", None), P("x", None), P(), P()),
        out_specs=(P(None, BAND, "x", None), P(), P()),
        check_vma=False,
    )
```

```python
import functools

import jax
import jax.numpy as jnp
import numpy as np
from jax import lax
from jax.experimental import pallas as pl
from jax.experimental.pallas import tpu as pltpu
from jax.sharding import Mesh
from jax.sharding import PartitionSpec as P

BAND = ("y", "z", "c")
M = 256
F32 = jnp.float32
BF16 = jnp.bfloat16


def hi_lo(table):
    hi = table.astype(np.float32).astype(jnp.bfloat16)
    lo = (table - hi.astype(np.float64)).astype(np.float32).astype(jnp.bfloat16)
    return np.stack([hi, lo])


def tables(points, radius):
    freq = np.arange(2 * radius) - radius + 1
    pos = np.arange(M)
    ang = 2.0 * np.pi * ((freq[:, None] * pos[None, :]) % M) / M
    cos, sin = np.cos(ang), np.sin(ang)
    wz = np.block([[cos, sin], [-sin, cos]])
    top = 2 * radius - 2
    q = np.arange(1, top + 1)
    shift = pos[:, None] / M - np.arange(points)[None, :] / points
    resample = np.ones((M, points))
    for k in q:
        resample += 2.0 * np.cos(2.0 * np.pi * k * shift)
    resample /= points
    return hi_lo(wz), hi_lo(wz.T), hi_lo(resample.T), hi_lo(resample)


def split(x):
    hi = x.astype(BF16)
    return hi, (x - hi.astype(F32)).astype(BF16)


def mm(a, b):
    return lax.dot_general(a, b, (((1,), (0,)), ((), ())), preferred_element_type=F32)


def mm_nt(a, b):
    return lax.dot_general(a, b, (((1,), (1,)), ((), ())), preferred_element_type=F32)


def first_kernel(ent_hbm, orb_hbm, pot_hbm, bx_hbm, zmsg_ref, packed_ref, ent_s, orb_s, pot_s, bx_s, sems):
    first = pl.multiple_of(lax.axis_index("x") * 40, 8)
    copies = [
        pltpu.make_async_copy(src, dst, sems.at[i])
        for i, (src, dst) in enumerate(
            [(ent_hbm.at[pl.ds(first, 40), :], ent_s), (orb_hbm, orb_s), (bx_hbm, bx_s), (pot_hbm, pot_s)]
        )
    ]
    for copy in copies:
        copy.start()
    copies[0].wait()
    copies[1].wait()
    ent_t = ent_s[...].T
    orb = orb_s[...].astype(F32)
    lane = lax.broadcasted_iota(jnp.int32, (128, 128), 1)
    sub = lax.broadcasted_iota(jnp.int32, (128, 128), 0)
    pieces = [[], []]
    for g in range(5):
        rows = []
        for r in range(8):
            s = 8 * g + r
            match = ent_t[:, s : s + 1] == lane
            rows.append(jnp.max(jnp.where(match, sub, -1), axis=0, keepdims=True))
        source = jnp.concatenate(rows, axis=0)
        index = jnp.maximum(source, 0)
        for c in range(2):
            moved = jnp.take_along_axis(orb[c, 8 * g : 8 * g + 8, :], index, axis=1)
            pieces[c].append(jnp.where(source >= 0, moved, 0.0))
    spread = jnp.concatenate(pieces[0] + pieces[1], axis=0).astype(BF16)
    for z in range(12):
        zmsg_ref[z] = spread
    packed_ref[0:80, :] = spread
    copies[2].wait()
    copies[3].wait()
    v_hi, v_lo = split(pot_s[...])
    vx = mm(v_hi, bx_s[0]) + mm(v_lo, bx_s[0]) + mm(v_hi, bx_s[1])
    vx = jnp.concatenate([vx[:, :128], vx[:, 128:]], axis=0)
    hi, lo = split(vx)
    packed_ref[80:320, :] = hi
    packed_ref[320:560, :] = lo


def main_kernel(all_ref, ent_ref, slot_row_ref, slot_col_ref, wz_ref, wx_ref, bz_ref, h_ref, out_ref):
    d = lax.axis_index("x")
    first = pl.multiple_of(d * 40, 8)

    def rows_of_all(start, count):
        return jnp.concatenate([all_ref[d, start : start + count, :].astype(F32) for d in range(4)], axis=0)

    def gathered_v(start):
        halves = [rows_of_all(start, 120), rows_of_all(start + 120, 120)]
        return jnp.concatenate(halves, axis=1).astype(BF16)

    v_hi = gathered_v(80)
    v_lo = gathered_v(320)
    pot = mm(bz_ref[0], v_hi) + mm(bz_ref[1], v_hi) + mm(bz_ref[0], v_lo)
    pot = pot.T

    place = (
        lax.broadcasted_iota(jnp.int32, (128, 160), 0) == jnp.broadcast_to(slot_row_ref[...], (128, 160))
    ).astype(F32).astype(BF16)
    c_re = rows_of_all(0, 40).astype(BF16)
    c_im = rows_of_all(40, 40).astype(BF16)
    sticks = jnp.concatenate([mm(place, c_re), mm(place, c_im)], axis=0).astype(BF16)

    t = mm(wx_ref[0], sticks) + mm(wx_ref[1], sticks)
    t = jnp.concatenate([t[:M], t[M:]], axis=1)
    t_hi, t_lo = split(t)
    field = mm(t_hi, wz_ref[0]) + mm(t_lo, wz_ref[0]) + mm(t_hi, wz_ref[1])
    prod = jnp.concatenate([field[:, :M] * pot, field[:, M:] * pot], axis=1)
    p_hi, p_lo = split(prod)
    y = mm(p_hi, wx_ref[0]) + mm(p_lo, wx_ref[0]) + mm(p_hi, wx_ref[1])
    y = jnp.concatenate([y[:, :128], y[:, 128:]], axis=0)
    y_hi, y_lo = split(y)

    slot = slot_col_ref[pl.ds(first, 40), :]
    pick = (lax.broadcasted_iota(jnp.int32, (40, 128), 1) == slot).astype(F32)
    none = jnp.zeros((40, 128), F32)
    pick = jnp.concatenate(
        [jnp.concatenate([pick, none], axis=1), jnp.concatenate([none, pick], axis=1)], axis=0
    ).astype(BF16)
    w_hi = mm(pick, wz_ref[0]).astype(BF16)
    w_lo = mm(pick, wz_ref[1]).astype(BF16)
    applied = (mm(w_hi, y_hi) + mm(w_hi, y_lo) + mm(w_lo, y_hi)) * (1.0 / (M * M))

    gx = slot - 63
    gz = lax.broadcasted_iota(jnp.int32, (40, 128), 1) - 63
    square = gx * gx + gz * gz
    inside = (square < 64 * 64) & (slot >= 0)
    kinetic = square.astype(F32) * (1.0 / 4096.0)
    own = all_ref[d, 0:80, :].astype(F32)
    ent = ent_ref[pl.ds(first, 40), :]
    index = jnp.maximum(ent, 0)
    for c in range(2):
        value = kinetic * own[40 * c : 40 * c + 40] + applied[40 * c : 40 * c + 40]
        h = jnp.where(inside, value, 0.0).astype(BF16).astype(F32)
        h_ref[40 * c : 40 * c + 40, :] = h
        moved = [jnp.take_along_axis(h[8 * g : 8 * g + 8], index[8 * g : 8 * g + 8], axis=1) for g in range(5)]
        out_ref[c] = jnp.where(ent >= 0, jnp.concatenate(moved, axis=0), 0.0).astype(BF16)


def message_kernel(psi_ref, h_ref, msg_ref, psi_s):
    for z in range(12):
        psi_s[80 * z : 80 * z + 80, :] = psi_ref[z].astype(F32)
    for y in range(8):
        rows = [psi_s[pl.ds(y, 120, stride=8), :], h_ref[pl.ds(y, 10, stride=8), :], jnp.zeros((14, 128), F32)]
        msg_ref[y] = jnp.concatenate(rows, axis=0).astype(BF16)


def product_kernel(both_ref, own_ref, block_ref, all_s, own_s, psi_s):
    for c in range(2):
        for y in range(8):
            at = (8 * c + y) * 144
            all_s[at : at + 144, :] = both_ref[c, y].astype(F32)
            for q in range(10):
                psi_s[q, pl.ds(24 * y + c, 12, stride=2), :] = all_s[pl.ds(at + q, 12, stride=10), :]
    for y in range(8):
        own_s[144 * y : 144 * y + 144, :] = own_ref[y].astype(F32)

    def entries(first):
        rows = [own_s[pl.ds(first + r, 8, stride=144), :] for r in range(5)]
        return jnp.concatenate(rows, axis=1)

    z = lax.axis_index("z") * 10
    m_re, m_im = entries(z), entries(z + 5)
    a_re, a_im = entries(120), entries(125)
    left_re = jnp.concatenate([m_re, m_im, a_re, a_im], axis=0).astype(BF16)
    left_im = jnp.concatenate([m_im, -m_re, a_im, -a_re], axis=0).astype(BF16)
    p_re = jnp.concatenate([psi_s[r] for r in range(5)], axis=1).astype(BF16)
    p_im = jnp.concatenate([psi_s[5 + r] for r in range(5)], axis=1).astype(BF16)
    block = (mm_nt(left_re, p_re) + mm_nt(left_im, p_im)) * (1.0 / 16384.0)
    for x in range(4):
        block_ref[x, 0:32, :] = block[:, :128]
        block_ref[x, 32:48, :] = jnp.concatenate([block[:16, 128:], block[16:, 128:]], axis=1)


def last_kernel(all_ref, s_ref, h_ref, t_s):
    for c in range(2):
        for z in range(12):
            tail = all_ref[c, z, 32:48, :]
            for m in range(4):
                rows = pl.ds(z * 2 + c, 8, stride=24)
                t_s[2 * m, rows, :] = all_ref[c, z, 8 * m : 8 * m + 8, :]
                half = tail[8 * (m % 2) : 8 * (m % 2) + 8]
                if m >= 2:
                    half = jnp.concatenate([half[:, 64:], half[:, :64]], axis=1)
                t_s[2 * m + 1, rows, :] = half
    for m in range(4):
        ref = s_ref if m < 2 else h_ref
        ref[m % 2, 0:128, :] = t_s[2 * m].T
        ref[m % 2, 128:192, :] = t_s[2 * m + 1].T[:64]


def call(kernel, outs, *args, scratch=(), hbm=False):
    space = {"in_specs": [pl.BlockSpec(memory_space=pltpu.HBM)] * len(args)} if hbm else {}
    if hbm:
        args = [pltpu.with_memory_space_constraint(a, pltpu.HBM) for a in args]
    return pl.pallas_call(
        kernel,
        out_shape=outs,
        scratch_shapes=list(scratch),
        compiler_params=pltpu.CompilerParams(vmem_limit_bytes=48 * 1024 * 1024),
        **space,
    )(*args)


def shape(dims, dtype):
    return jax.ShapeDtypeStruct(dims, dtype)


def body(orbitals, potential, slot_sticks, stick_entries):
    wz, wx, bx, bz = tables(potential.shape[1], 64)
    zmsg, packed = call(
        first_kernel,
        [shape((12, 80, 128), BF16), shape((560, 128), BF16)],
        stick_entries, orbitals.reshape(2, 40, 128), potential, bx,
        scratch=[
            pltpu.VMEM((40, 128), jnp.int32),
            pltpu.VMEM((2, 40, 128), BF16),
            pltpu.VMEM((120, 480), F32),
            pltpu.VMEM((2, 480, 256), BF16),
            pltpu.SemaphoreType.DMA((4,)),
        ],
        hbm=True,
    )
    psi = lax.all_to_all(zmsg, "z", 0, 0, tiled=True)
    everyone = lax.all_gather(packed, "x")
    h, out = call(
        main_kernel,
        [shape((80, 128), F32), shape((2, 40, 128), BF16)],
        everyone, stick_entries, slot_sticks.reshape(1, 160), slot_sticks.reshape(160, 1), wz, wx, bz,
    )
    msg = call(message_kernel, shape((8, 144, 128), BF16), psi, h, scratch=[pltpu.VMEM((960, 128), F32)])
    arrived = lax.all_to_all(msg, "y", 0, 0, tiled=True)
    both = lax.all_gather(arrived, "c")
    block = call(
        product_kernel,
        shape((4, 48, 128), F32),
        both, arrived,
        scratch=[pltpu.VMEM((2304, 128), F32), pltpu.VMEM((1152, 128), F32), pltpu.VMEM((10, 192, 128), F32)],
    )
    block = lax.all_to_all(block, "x", 0, 0, tiled=True).sum(axis=0)
    block = lax.all_to_all(jnp.broadcast_to(block, (8, 48, 128)), "y", 0, 0, tiled=True).sum(axis=0)
    block = lax.all_to_all(jnp.broadcast_to(block, (12, 48, 128)), "z", 0, 0, tiled=True)
    correlation, reduced = call(
        last_kernel,
        [shape((2, 192, 192), F32), shape((2, 192, 192), F32)],
        lax.all_gather(block, "c"),
        scratch=[pltpu.VMEM((8, 192, 128), F32)],
    )
    return out.reshape(orbitals.shape), correlation, reduced


def solution(mesh):
    finer = Mesh(mesh.devices.reshape(8, 12, 2, mesh.shape["ga"]), ("y", "z", "c", "x"))
    return jax.shard_map(
        body,
        mesh=finer,
        in_specs=(P(None, BAND, "x", None), P("x", None), P(), P()),
        out_specs=(P(None, BAND, "x", None), P(), P()),
        check_vma=False,
    )
```

```python
import functools

import jax
import jax.numpy as jnp
import numpy as np
from jax import lax
from jax.experimental import pallas as pl
from jax.experimental.pallas import tpu as pltpu
from jax.sharding import Mesh
from jax.sharding import PartitionSpec as P

BAND = ("y", "z", "c")
M = 256
F32 = jnp.float32
BF16 = jnp.bfloat16


def hi_lo(table):
    hi = table.astype(np.float32).astype(jnp.bfloat16)
    lo = (table - hi.astype(np.float64)).astype(np.float32).astype(jnp.bfloat16)
    return np.stack([hi, lo])


def tables(points, radius):
    freq = np.arange(2 * radius) - radius + 1
    pos = np.arange(M)
    ang = 2.0 * np.pi * ((freq[:, None] * pos[None, :]) % M) / M
    cos, sin = np.cos(ang), np.sin(ang)
    wz = np.block([[cos, sin], [-sin, cos]])
    top = 2 * radius - 2
    q = np.arange(1, top + 1)
    shift = pos[:, None] / M - np.arange(points)[None, :] / points
    resample = np.ones((M, points))
    for k in q:
        resample += 2.0 * np.cos(2.0 * np.pi * k * shift)
    resample /= points
    return hi_lo(wz), hi_lo(wz.T), hi_lo(resample.T), hi_lo(resample)


def split(x):
    hi = x.astype(BF16)
    return hi, (x - hi.astype(F32)).astype(BF16)


def mm(a, b):
    return lax.dot_general(a, b, (((1,), (0,)), ((), ())), preferred_element_type=F32)


def mm_nt(a, b):
    return lax.dot_general(a, b, (((1,), (1,)), ((), ())), preferred_element_type=F32)


def first_kernel(ent_hbm, orb_hbm, pot_hbm, bx_hbm, zmsg_ref, packed_ref, ent_s, orb_s, pot_s, bx_s, sems):
    first = pl.multiple_of(lax.axis_index("x") * 40, 8)
    copies = [
        pltpu.make_async_copy(src, dst, sems.at[i])
        for i, (src, dst) in enumerate(
            [(ent_hbm.at[pl.ds(first, 40), :], ent_s), (orb_hbm, orb_s), (bx_hbm, bx_s), (pot_hbm, pot_s)]
        )
    ]
    for copy in copies:
        copy.start()
    copies[0].wait()
    copies[1].wait()
    ent_t = ent_s[...].T
    orb = orb_s[...].astype(F32)
    lane = lax.broadcasted_iota(jnp.int32, (128, 128), 1)
    sub = lax.broadcasted_iota(jnp.int32, (128, 128), 0)
    pieces = [[], []]
    for g in range(5):
        rows = []
        for r in range(8):
            s = 8 * g + r
            match = ent_t[:, s : s + 1] == lane
            rows.append(jnp.max(jnp.where(match, sub, -1), axis=0, keepdims=True))
        source = jnp.concatenate(rows, axis=0)
        index = jnp.maximum(source, 0)
        for c in range(2):
            moved = jnp.take_along_axis(orb[c, 8 * g : 8 * g + 8, :], index, axis=1)
            pieces[c].append(jnp.where(source >= 0, moved, 0.0))
    spread = jnp.concatenate(pieces[0] + pieces[1], axis=0).astype(BF16)
    for z in range(12):
        zmsg_ref[z] = spread
    packed_ref[0:80, :] = spread
    copies[2].wait()
    copies[3].wait()
    v_hi, v_lo = split(pot_s[...])
    vx = mm(v_hi, bx_s[0]) + mm(v_lo, bx_s[0]) + mm(v_hi, bx_s[1])
    vx = jnp.concatenate([vx[:, :128], vx[:, 128:]], axis=0)
    hi, lo = split(vx)
    packed_ref[80:320, :] = hi
    packed_ref[320:560, :] = lo


def main_kernel(all_ref, ent_ref, slot_row_ref, slot_col_ref, wz_ref, wx_ref, bz_ref, msg_ref, out_ref):
    d = lax.axis_index("x")
    first = pl.multiple_of(d * 40, 8)

    def rows_of_all(start, count):
        return jnp.concatenate([all_ref[d, start : start + count, :].astype(F32) for d in range(4)], axis=0)

    def gathered_v(start):
        halves = [rows_of_all(start, 120), rows_of_all(start + 120, 120)]
        return jnp.concatenate(halves, axis=1).astype(BF16)

    v_hi = gathered_v(80)
    v_lo = gathered_v(320)
    pot = mm(bz_ref[0], v_hi) + mm(bz_ref[1], v_hi) + mm(bz_ref[0], v_lo)
    pot = pot.T

    place = (
        lax.broadcasted_iota(jnp.int32, (128, 160), 0) == jnp.broadcast_to(slot_row_ref[...], (128, 160))
    ).astype(F32).astype(BF16)
    c_re = rows_of_all(0, 40).astype(BF16)
    c_im = rows_of_all(40, 40).astype(BF16)
    sticks = jnp.concatenate([mm(place, c_re), mm(place, c_im)], axis=0).astype(BF16)

    t = mm(wx_ref[0], sticks) + mm(wx_ref[1], sticks)
    t = jnp.concatenate([t[:M], t[M:]], axis=1)
    t_hi, t_lo = split(t)
    field = mm(t_hi, wz_ref[0]) + mm(t_lo, wz_ref[0]) + mm(t_hi, wz_ref[1])
    prod = jnp.concatenate([field[:, :M] * pot, field[:, M:] * pot], axis=1)
    p_hi, p_lo = split(prod)
    y = mm(p_hi, wx_ref[0]) + mm(p_lo, wx_ref[0]) + mm(p_hi, wx_ref[1])
    y = jnp.concatenate([y[:, :128], y[:, 128:]], axis=0)
    y_hi, y_lo = split(y)

    slot = slot_col_ref[pl.ds(first, 40), :]
    pick = (lax.broadcasted_iota(jnp.int32, (40, 128), 1) == slot).astype(F32)
    none = jnp.zeros((40, 128), F32)
    pick = jnp.concatenate(
        [jnp.concatenate([pick, none], axis=1), jnp.concatenate([none, pick], axis=1)], axis=0
    ).astype(BF16)
    w_hi = mm(pick, wz_ref[0]).astype(BF16)
    w_lo = mm(pick, wz_ref[1]).astype(BF16)
    applied = (mm(w_hi, y_hi) + mm(w_hi, y_lo) + mm(w_lo, y_hi)) * (1.0 / (M * M))

    gx = slot - 63
    gz = lax.broadcasted_iota(jnp.int32, (40, 128), 1) - 63
    square = gx * gx + gz * gz
    inside = (square < 64 * 64) & (slot >= 0)
    kinetic = square.astype(F32) * (1.0 / 4096.0)
    own = all_ref[d, 0:80, :].astype(F32)
    ent = ent_ref[pl.ds(first, 40), :]
    index = jnp.maximum(ent, 0)
    message = [own]
    for c in range(2):
        value = kinetic * own[40 * c : 40 * c + 40] + applied[40 * c : 40 * c + 40]
        h = jnp.where(inside, value, 0.0).astype(BF16).astype(F32)
        message.append(h)
        moved = [jnp.take_along_axis(h[8 * g : 8 * g + 8], index[8 * g : 8 * g + 8], axis=1) for g in range(5)]
        out_ref[c] = jnp.where(ent >= 0, jnp.concatenate(moved, axis=0), 0.0).astype(BF16)
    message = jnp.concatenate(message, axis=0).astype(BF16)
    for y in range(8):
        msg_ref[y] = message


def rows_kernel(psi_ref, p_ref, psi_s):
    for c in range(2):
        for z in range(12):
            at = (2 * z + c) * 80
            psi_s[at : at + 80, :] = psi_ref[c, z].astype(F32)
    pad = jnp.zeros((8, 128), F32)
    for part in range(2):
        for s in range(40):
            block = jnp.concatenate([psi_s[pl.ds(40 * part + s, 24, stride=80), :], pad], axis=0)
            p_ref[part, :, 128 * s : 128 * s + 128] = block.astype(BF16)


def product_kernel(p_ref, own_ref, block_ref, own_s):
    for y in range(8):
        own_s[160 * y : 160 * y + 160, :] = own_ref[y].astype(F32)

    def entries(first):
        rows = [own_s[pl.ds(first + s, 8, stride=160), :] for s in range(40)]
        return jnp.concatenate(rows, axis=1)

    m_re, m_im, a_re, a_im = [entries(40 * q) for q in range(4)]
    left_re = jnp.concatenate([m_re, m_im, a_re, a_im], axis=0).astype(BF16)
    left_im = jnp.concatenate([m_im, -m_re, a_im, -a_re], axis=0).astype(BF16)
    block = (mm_nt(left_re, p_ref[0]) + mm_nt(left_im, p_ref[1])) * (1.0 / 16384.0)
    row = [block[8 * m : 8 * m + 8, :24] for m in range(4)] + [jnp.zeros((8, 32), F32)]
    row = jnp.concatenate(row, axis=1)
    for x in range(4):
        block_ref[x] = row


def pack_kernel(blocks_ref, packed_ref):
    row = jnp.concatenate([blocks_ref[z][:, :96] for z in range(12)], axis=1)
    for y in range(8):
        packed_ref[y] = row


def last_kernel(all_ref, s_ref, h_ref, t_s):
    for c in range(2):
        for z in range(12):
            for m in range(4):
                at = 96 * z + 24 * m
                row = jnp.concatenate([all_ref[c, y, :, at : at + 24] for y in range(8)], axis=1)
                rows = pl.ds(z * 2 + c, 8, stride=24)
                t_s[2 * m, rows, :] = row[:, :128]
                t_s[2 * m + 1, rows, 0:64] = row[:, 128:]
    for m in range(4):
        ref = s_ref if m < 2 else h_ref
        ref[m % 2, 0:128, :] = t_s[2 * m].T
        ref[m % 2, 128:192, :] = t_s[2 * m + 1].T[:64]


def call(kernel, outs, *args, scratch=(), hbm=False):
    space = {"in_specs": [pl.BlockSpec(memory_space=pltpu.HBM)] * len(args)} if hbm else {}
    if hbm:
        args = [pltpu.with_memory_space_constraint(a, pltpu.HBM) for a in args]
    return pl.pallas_call(
        kernel,
        out_shape=outs,
        scratch_shapes=list(scratch),
        compiler_params=pltpu.CompilerParams(vmem_limit_bytes=48 * 1024 * 1024),
        **space,
    )(*args)


def shape(dims, dtype):
    return jax.ShapeDtypeStruct(dims, dtype)


def body(orbitals, potential, slot_sticks, stick_entries):
    wz, wx, bx, bz = tables(potential.shape[1], 64)
    zmsg, packed = call(
        first_kernel,
        [shape((12, 80, 128), BF16), shape((560, 128), BF16)],
        stick_entries, orbitals.reshape(2, 40, 128), potential, bx,
        scratch=[
            pltpu.VMEM((40, 128), jnp.int32),
            pltpu.VMEM((2, 40, 128), BF16),
            pltpu.VMEM((120, 480), F32),
            pltpu.VMEM((2, 480, 256), BF16),
            pltpu.SemaphoreType.DMA((4,)),
        ],
        hbm=True,
    )
    psi = lax.all_to_all(zmsg, "z", 0, 0, tiled=True)
    everyone = lax.all_gather(packed, "x")
    msg, out = call(
        main_kernel,
        [shape((8, 160, 128), BF16), shape((2, 40, 128), BF16)],
        everyone, stick_entries, slot_sticks.reshape(1, 160), slot_sticks.reshape(160, 1), wz, wx, bz,
    )
    own = lax.all_to_all(msg, "y", 0, 0, tiled=True)
    rows = call(
        rows_kernel, shape((2, 32, 5120), BF16), lax.all_gather(psi, "c"), scratch=[pltpu.VMEM((1920, 128), F32)]
    )
    block = call(product_kernel, shape((4, 8, 128), F32), rows, own, scratch=[pltpu.VMEM((1280, 128), F32)])
    block = lax.all_to_all(block, "x", 0, 0, tiled=True).sum(axis=0)
    blocks = lax.all_to_all(jnp.broadcast_to(block, (12, 8, 128)), "z", 0, 0, tiled=True)
    packed = call(pack_kernel, shape((8, 8, 1152), F32), blocks)
    packed = lax.all_to_all(packed, "y", 0, 0, tiled=True)
    correlation, reduced = call(
        last_kernel,
        [shape((2, 192, 192), F32), shape((2, 192, 192), F32)],
        lax.all_gather(packed, "c"),
        scratch=[pltpu.VMEM((8, 192, 128), F32)],
    )
    return out.reshape(orbitals.shape), correlation, reduced


def solution(mesh):
    finer = Mesh(mesh.devices.reshape(8, 12, 2, mesh.shape["ga"]), ("y", "z", "c", "x"))
    return jax.shard_map(
        body,
        mesh=finer,
        in_specs=(P(None, BAND, "x", None), P("x", None), P(), P()),
        out_specs=(P(None, BAND, "x", None), P(), P()),
        check_vma=False,
    )
```

```python
import functools

import jax
import jax.numpy as jnp
import numpy as np
from jax import lax
from jax.experimental import pallas as pl
from jax.experimental.pallas import tpu as pltpu
from jax.sharding import Mesh
from jax.sharding import PartitionSpec as P

BAND = ("y", "z", "c")
M = 256
F32 = jnp.float32
BF16 = jnp.bfloat16


def hi_lo(table):
    hi = table.astype(np.float32).astype(jnp.bfloat16)
    lo = (table - hi.astype(np.float64)).astype(np.float32).astype(jnp.bfloat16)
    return np.stack([hi, lo])


def tables(points, radius):
    freq = np.arange(2 * radius) - radius + 1
    pos = np.arange(M)
    ang = 2.0 * np.pi * ((freq[:, None] * pos[None, :]) % M) / M
    cos, sin = np.cos(ang), np.sin(ang)
    wz = np.block([[cos, sin], [-sin, cos]])
    top = 2 * radius - 2
    q = np.arange(1, top + 1)
    shift = pos[:, None] / M - np.arange(points)[None, :] / points
    resample = np.ones((M, points))
    for k in q:
        resample += 2.0 * np.cos(2.0 * np.pi * k * shift)
    resample /= points
    return hi_lo(wz), hi_lo(wz.T), hi_lo(resample.T), hi_lo(resample)


def split(x):
    hi = x.astype(BF16)
    return hi, (x - hi.astype(F32)).astype(BF16)


def mm(a, b):
    return lax.dot_general(a, b, (((1,), (0,)), ((), ())), preferred_element_type=F32)


def mm_nt(a, b):
    return lax.dot_general(a, b, (((1,), (1,)), ((), ())), preferred_element_type=F32)


def first_kernel(ent_hbm, orb_hbm, pot_hbm, bx_hbm, zmsg_hbm, packed_ref, ent_s, orb_s, pot_s, bx_s, sems):
    first = pl.multiple_of(lax.axis_index("x") * 40, 8)
    copies = [
        pltpu.make_async_copy(src, dst, sems.at[i])
        for i, (src, dst) in enumerate(
            [(ent_hbm.at[pl.ds(first, 40), :], ent_s), (orb_hbm, orb_s), (bx_hbm, bx_s), (pot_hbm, pot_s)]
        )
    ]
    for copy in copies:
        copy.start()
    copies[0].wait()
    copies[1].wait()
    ent_t = ent_s[...].T
    orb = orb_s[...].astype(F32)
    lane = lax.broadcasted_iota(jnp.int32, (128, 128), 1)
    sub = lax.broadcasted_iota(jnp.int32, (128, 128), 0)
    pieces = [[], []]
    for g in range(5):
        rows = []
        for r in range(8):
            s = 8 * g + r
            match = ent_t[:, s : s + 1] == lane
            rows.append(jnp.max(jnp.where(match, sub, -1), axis=0, keepdims=True))
        source = jnp.concatenate(rows, axis=0)
        index = jnp.maximum(source, 0)
        for c in range(2):
            moved = jnp.take_along_axis(orb[c, 8 * g : 8 * g + 8, :], index, axis=1)
            pieces[c].append(jnp.where(source >= 0, moved, 0.0))
    spread = jnp.concatenate(pieces[0] + pieces[1], axis=0).astype(BF16)
    packed_ref[0:80, :] = spread
    sends = [pltpu.make_async_copy(packed_ref.at[0:80, :], zmsg_hbm.at[z], sems.at[4 + z]) for z in range(12)]
    for send in sends:
        send.start()
    copies[2].wait()
    copies[3].wait()
    v_hi, v_lo = split(pot_s[...])
    vx = mm(v_hi, bx_s[0]) + mm(v_lo, bx_s[0]) + mm(v_hi, bx_s[1])
    vx = jnp.concatenate([vx[:, :128], vx[:, 128:]], axis=0)
    hi, lo = split(vx)
    packed_ref[80:320, :] = hi
    packed_ref[320:560, :] = lo
    for send in sends:
        send.wait()


def main_kernel(all_ref, ent_ref, slot_row_ref, slot_col_ref, wz_ref, wx_ref, bz_ref, msg_ref, out_ref):
    d = lax.axis_index("x")
    first = pl.multiple_of(d * 40, 8)

    def rows_of_all(start, count):
        return jnp.concatenate([all_ref[d, start : start + count, :].astype(F32) for d in range(4)], axis=0)

    def gathered_v(start):
        halves = [rows_of_all(start, 120), rows_of_all(start + 120, 120)]
        return jnp.concatenate(halves, axis=1).astype(BF16)

    v_hi = gathered_v(80)
    v_lo = gathered_v(320)
    pot = mm(bz_ref[0], v_hi) + mm(bz_ref[1], v_hi) + mm(bz_ref[0], v_lo)
    pot = pot.T

    place = (
        lax.broadcasted_iota(jnp.int32, (128, 160), 0) == jnp.broadcast_to(slot_row_ref[...], (128, 160))
    ).astype(F32).astype(BF16)
    c_re = rows_of_all(0, 40).astype(BF16)
    c_im = rows_of_all(40, 40).astype(BF16)
    sticks = jnp.concatenate([mm(place, c_re), mm(place, c_im)], axis=0).astype(BF16)

    t = mm(wx_ref[0], sticks) + mm(wx_ref[1], sticks)
    t = jnp.concatenate([t[:M], t[M:]], axis=1)
    t_hi, t_lo = split(t)
    field = mm(t_hi, wz_ref[0]) + mm(t_lo, wz_ref[0]) + mm(t_hi, wz_ref[1])
    prod = jnp.concatenate([field[:, :M] * pot, field[:, M:] * pot], axis=1)
    p_hi, p_lo = split(prod)
    y = mm(p_hi, wx_ref[0]) + mm(p_lo, wx_ref[0]) + mm(p_hi, wx_ref[1])
    y = jnp.concatenate([y[:, :128], y[:, 128:]], axis=0)
    y_hi, y_lo = split(y)

    slot = slot_col_ref[pl.ds(first, 40), :]
    pick = (lax.broadcasted_iota(jnp.int32, (40, 128), 1) == slot).astype(F32)
    none = jnp.zeros((40, 128), F32)
    pick = jnp.concatenate(
        [jnp.concatenate([pick, none], axis=1), jnp.concatenate([none, pick], axis=1)], axis=0
    ).astype(BF16)
    w_hi = mm(pick, wz_ref[0]).astype(BF16)
    w_lo = mm(pick, wz_ref[1]).astype(BF16)
    applied = (mm(w_hi, y_hi) + mm(w_hi, y_lo) + mm(w_lo, y_hi)) * (1.0 / (M * M))

    gx = slot - 63
    gz = lax.broadcasted_iota(jnp.int32, (40, 128), 1) - 63
    square = gx * gx + gz * gz
    inside = (square < 64 * 64) & (slot >= 0)
    kinetic = square.astype(F32) * (1.0 / 4096.0)
    own = all_ref[d, 0:80, :].astype(F32)
    ent = ent_ref[pl.ds(first, 40), :]
    index = jnp.maximum(ent, 0)
    message = [own]
    for c in range(2):
        value = kinetic * own[40 * c : 40 * c + 40] + applied[40 * c : 40 * c + 40]
        h = jnp.where(inside, value, 0.0).astype(BF16).astype(F32)
        message.append(h)
        moved = [jnp.take_along_axis(h[8 * g : 8 * g + 8], index[8 * g : 8 * g + 8], axis=1) for g in range(5)]
        out_ref[c] = jnp.where(ent >= 0, jnp.concatenate(moved, axis=0), 0.0).astype(BF16)
    message = jnp.concatenate(message, axis=0).astype(BF16)
    for y in range(8):
        msg_ref[y] = message


def rows_kernel(psi_ref, p_ref, psi_s):
    for c in range(2):
        for z in range(12):
            at = (2 * z + c) * 80
            psi_s[at : at + 80, :] = psi_ref[c, z].astype(F32)
    pad = jnp.zeros((8, 128), F32)
    for part in range(2):
        for s in range(40):
            block = jnp.concatenate([psi_s[pl.ds(40 * part + s, 24, stride=80), :], pad], axis=0)
            p_ref[part, :, 128 * s : 128 * s + 128] = block.astype(BF16)


def product_kernel(p_ref, own_ref, block_ref, own_s):
    for y in range(8):
        own_s[160 * y : 160 * y + 160, :] = own_ref[y].astype(F32)

    def entries(first):
        rows = [own_s[pl.ds(first + s, 8, stride=160), :] for s in range(40)]
        return jnp.concatenate(rows, axis=1)

    m_re, m_im, a_re, a_im = [entries(40 * q) for q in range(4)]
    left_re = jnp.concatenate([m_re, m_im, a_re, a_im], axis=0).astype(BF16)
    left_im = jnp.concatenate([m_im, -m_re, a_im, -a_re], axis=0).astype(BF16)
    block = (mm_nt(left_re, p_ref[0]) + mm_nt(left_im, p_ref[1])) * (1.0 / 16384.0)
    row = [block[8 * m : 8 * m + 8, :24] for m in range(4)] + [jnp.zeros((8, 32), F32)]
    row = jnp.concatenate(row, axis=1)
    for peer in range(32):
        block_ref[peer] = row


def join_kernel(blocks_ref, joined_ref):
    sums = [(blocks_ref[y, 0] + blocks_ref[y, 1]) + (blocks_ref[y, 2] + blocks_ref[y, 3]) for y in range(8)]
    block = [jnp.concatenate([sums[y][:, 24 * m : 24 * m + 24] for y in range(8)], axis=1) for m in range(4)]
    tail = [
        jnp.concatenate([block[0][:, 128:], block[2][:, 128:]], axis=1),
        jnp.concatenate([block[1][:, 128:], block[3][:, 128:]], axis=1),
    ]
    joined = jnp.concatenate([b[:, :128] for b in block] + tail, axis=0)
    for z in range(12):
        joined_ref[z] = joined


def last_kernel(all_ref, s_ref, h_ref, t_s):
    for c in range(2):
        for z in range(12):
            rows = pl.ds(z * 2 + c, 8, stride=24)
            tail = all_ref[c, z, 32:48, :]
            swapped = jnp.concatenate([tail[:, 64:], tail[:, :64]], axis=1)
            for m in range(4):
                t_s[2 * m, rows, :] = all_ref[c, z, 8 * m : 8 * m + 8, :]
                half = swapped if m >= 2 else tail
                t_s[2 * m + 1, rows, :] = half[8 * (m % 2) : 8 * (m % 2) + 8]
    for m in range(4):
        ref = s_ref if m < 2 else h_ref
        ref[m % 2, 0:128, :] = t_s[2 * m].T
        ref[m % 2, 128:192, :] = t_s[2 * m + 1].T[:64]


def call(kernel, outs, *args, scratch=(), hbm=False, **space):
    if hbm:
        space["in_specs"] = [pl.BlockSpec(memory_space=pltpu.HBM)] * len(args)
        args = [pltpu.with_memory_space_constraint(a, pltpu.HBM) for a in args]
    return pl.pallas_call(
        kernel,
        out_shape=outs,
        scratch_shapes=list(scratch),
        compiler_params=pltpu.CompilerParams(vmem_limit_bytes=48 * 1024 * 1024),
        **space,
    )(*args)


def shape(dims, dtype):
    return jax.ShapeDtypeStruct(dims, dtype)


def body(orbitals, potential, slot_sticks, stick_entries):
    wz, wx, bx, bz = tables(potential.shape[1], 64)
    zmsg, packed = call(
        first_kernel,
        [shape((12, 80, 128), BF16), shape((560, 128), BF16)],
        stick_entries, orbitals.reshape(2, 40, 128), potential, bx,
        scratch=[
            pltpu.VMEM((40, 128), jnp.int32),
            pltpu.VMEM((2, 40, 128), BF16),
            pltpu.VMEM((120, 480), F32),
            pltpu.VMEM((2, 480, 256), BF16),
            pltpu.SemaphoreType.DMA((16,)),
        ],
        hbm=True,
        out_specs=[pl.BlockSpec(memory_space=pltpu.HBM), pl.BlockSpec(memory_space=pltpu.VMEM)],
    )
    psi = lax.all_to_all(zmsg, "z", 0, 0, tiled=True)
    everyone = lax.all_gather(packed, "x")
    msg, out = call(
        main_kernel,
        [shape((8, 160, 128), BF16), shape((2, 40, 128), BF16)],
        everyone, stick_entries, slot_sticks.reshape(1, 160), slot_sticks.reshape(160, 1), wz, wx, bz,
    )
    own = lax.all_to_all(msg, "y", 0, 0, tiled=True)
    rows = call(
        rows_kernel, shape((2, 32, 5120), BF16), lax.all_gather(psi, "c"), scratch=[pltpu.VMEM((1920, 128), F32)]
    )
    block = call(product_kernel, shape((32, 8, 128), F32), rows, own, scratch=[pltpu.VMEM((1280, 128), F32)])
    blocks = lax.all_to_all(block, ("y", "x"), 0, 0, tiled=True)
    joined = call(join_kernel, shape((12, 48, 128), F32), blocks.reshape(8, 4, 8, 128))
    joined = lax.all_to_all(joined, "z", 0, 0, tiled=True)
    correlation, reduced = call(
        last_kernel,
        [shape((2, 192, 192), F32), shape((2, 192, 192), F32)],
        lax.all_gather(joined, "c"),
        scratch=[pltpu.VMEM((8, 192, 128), F32)],
    )
    return out.reshape(orbitals.shape), correlation, reduced


def solution(mesh):
    finer = Mesh(mesh.devices.reshape(8, 12, 2, mesh.shape["ga"]), ("y", "z", "c", "x"))
    return jax.shard_map(
        body,
        mesh=finer,
        in_specs=(P(None, BAND, "x", None), P("x", None), P(), P()),
        out_specs=(P(None, BAND, "x", None), P(), P()),
        check_vma=False,
    )
```

```python
import functools

import jax
import jax.numpy as jnp
import numpy as np
from jax import lax
from jax.experimental import pallas as pl
from jax.experimental.pallas import tpu as pltpu
from jax.sharding import Mesh
from jax.sharding import PartitionSpec as P

BAND = ("y", "z", "c")
M = 256
F32 = jnp.float32
BF16 = jnp.bfloat16


def hi_lo(table):
    hi = table.astype(np.float32).astype(jnp.bfloat16)
    lo = (table - hi.astype(np.float64)).astype(np.float32).astype(jnp.bfloat16)
    return np.stack([hi, lo])


def tables(points, radius):
    freq = np.arange(2 * radius) - radius + 1
    pos = np.arange(M)
    ang = 2.0 * np.pi * ((freq[:, None] * pos[None, :]) % M) / M
    cos, sin = np.cos(ang), np.sin(ang)
    wz = np.block([[cos, sin], [-sin, cos]])
    top = 2 * radius - 2
    q = np.arange(1, top + 1)
    shift = pos[:, None] / M - np.arange(points)[None, :] / points
    resample = np.ones((M, points))
    for k in q:
        resample += 2.0 * np.cos(2.0 * np.pi * k * shift)
    resample /= points
    return hi_lo(wz), hi_lo(wz.T), hi_lo(resample.T), hi_lo(resample)


def split(x):
    hi = x.astype(BF16)
    return hi, (x - hi.astype(F32)).astype(BF16)


def mm(a, b):
    return lax.dot_general(a, b, (((1,), (0,)), ((), ())), preferred_element_type=F32)


def mm_nt(a, b):
    return lax.dot_general(a, b, (((1,), (1,)), ((), ())), preferred_element_type=F32)


def first_kernel(ent_ref, orb_ref, pot_ref, bx_ref, packed_ref):
    first = pl.multiple_of(lax.axis_index("x") * 40, 8)
    ent_t = ent_ref[pl.ds(first, 40), :].T
    orb = orb_ref[...].astype(F32)
    lane = lax.broadcasted_iota(jnp.int32, (128, 128), 1)
    sub = lax.broadcasted_iota(jnp.int32, (128, 128), 0)
    pieces = [[], []]
    for g in range(5):
        rows = []
        for r in range(8):
            s = 8 * g + r
            match = ent_t[:, s : s + 1] == lane
            rows.append(jnp.max(jnp.where(match, sub, -1), axis=0, keepdims=True))
        source = jnp.concatenate(rows, axis=0)
        index = jnp.maximum(source, 0)
        for c in range(2):
            moved = jnp.take_along_axis(orb[c, 8 * g : 8 * g + 8, :], index, axis=1)
            pieces[c].append(jnp.where(source >= 0, moved, 0.0))
    spread = jnp.concatenate(pieces[0] + pieces[1], axis=0).astype(BF16)
    packed_ref[0:80, :] = spread
    v_hi, v_lo = split(pot_ref[...])
    vx = mm(v_hi, bx_ref[0]) + mm(v_lo, bx_ref[0]) + mm(v_hi, bx_ref[1])
    vx = jnp.concatenate([vx[:, :128], vx[:, 128:]], axis=0)
    hi, lo = split(vx)
    packed_ref[80:320, :] = hi
    packed_ref[320:560, :] = lo


def main_kernel(all_ref, orb_ref, ent_ref, slot_row_ref, slot_col_ref, wz_ref, wx_ref, bz_ref, msg_ref, out_ref):
    d = lax.axis_index("x")
    first = pl.multiple_of(d * 40, 8)

    def rows_of_all(start, count):
        return jnp.concatenate([all_ref[d, start : start + count, :].astype(F32) for d in range(4)], axis=0)

    def gathered_v(start):
        halves = [rows_of_all(start, 120), rows_of_all(start + 120, 120)]
        return jnp.concatenate(halves, axis=1).astype(BF16)

    v_hi = gathered_v(80)
    v_lo = gathered_v(320)
    pot = mm(bz_ref[0], v_hi) + mm(bz_ref[1], v_hi) + mm(bz_ref[0], v_lo)
    pot = pot.T

    place = (
        lax.broadcasted_iota(jnp.int32, (128, 160), 0) == jnp.broadcast_to(slot_row_ref[...], (128, 160))
    ).astype(F32).astype(BF16)
    c_re = rows_of_all(0, 40).astype(BF16)
    c_im = rows_of_all(40, 40).astype(BF16)
    sticks = jnp.concatenate([mm(place, c_re), mm(place, c_im)], axis=0).astype(BF16)

    t = mm(wx_ref[0], sticks) + mm(wx_ref[1], sticks)
    t = jnp.concatenate([t[:M], t[M:]], axis=1)
    t_hi, t_lo = split(t)
    field = mm(t_hi, wz_ref[0]) + mm(t_lo, wz_ref[0]) + mm(t_hi, wz_ref[1])
    prod = jnp.concatenate([field[:, :M] * pot, field[:, M:] * pot], axis=1)
    p_hi, p_lo = split(prod)
    y = mm(p_hi, wx_ref[0]) + mm(p_lo, wx_ref[0]) + mm(p_hi, wx_ref[1])
    y = jnp.concatenate([y[:, :128], y[:, 128:]], axis=0)
    y_hi, y_lo = split(y)

    slot = slot_col_ref[pl.ds(first, 40), :]
    pick = (lax.broadcasted_iota(jnp.int32, (40, 128), 1) == slot).astype(F32)
    none = jnp.zeros((40, 128), F32)
    pick = jnp.concatenate(
        [jnp.concatenate([pick, none], axis=1), jnp.concatenate([none, pick], axis=1)], axis=0
    ).astype(BF16)
    w_hi = mm(pick, wz_ref[0]).astype(BF16)
    w_lo = mm(pick, wz_ref[1]).astype(BF16)
    applied = (mm(w_hi, y_hi) + mm(w_hi, y_lo) + mm(w_lo, y_hi)) * (1.0 / (M * M))

    gx = slot - 63
    gz = lax.broadcasted_iota(jnp.int32, (40, 128), 1) - 63
    square = gx * gx + gz * gz
    inside = (square < 64 * 64) & (slot >= 0)
    kinetic = square.astype(F32) * (1.0 / 4096.0)
    own = all_ref[d, 0:80, :].astype(F32)
    ent = ent_ref[pl.ds(first, 40), :]
    index = jnp.maximum(ent, 0)
    masked, applied_rows = [], []
    for c in range(2):
        value = kinetic * own[40 * c : 40 * c + 40] + applied[40 * c : 40 * c + 40]
        h = jnp.where(inside, value, 0.0).astype(BF16).astype(F32)
        moved = [jnp.take_along_axis(h[8 * g : 8 * g + 8], index[8 * g : 8 * g + 8], axis=1) for g in range(5)]
        applied_rows.append(jnp.where(ent >= 0, jnp.concatenate(moved, axis=0), 0.0))
        masked.append(jnp.where(ent >= 0, orb_ref[c].astype(F32), 0.0))
        out_ref[c] = applied_rows[c].astype(BF16)
    message = jnp.concatenate(masked + applied_rows, axis=0).astype(BF16)
    for y in range(8):
        msg_ref[y] = message


def rows_kernel(psi_ref, p_ref, psi_s):
    for c in range(2):
        for z in range(12):
            at = (2 * z + c) * 80
            psi_s[at : at + 80, :] = psi_ref[c, z].astype(F32)
    pad = jnp.zeros((8, 128), F32)
    for part in range(2):
        for s in range(40):
            block = jnp.concatenate([psi_s[pl.ds(40 * part + s, 24, stride=80), :], pad], axis=0)
            p_ref[part, :, 128 * s : 128 * s + 128] = block.astype(BF16)


def product_kernel(p_ref, own_ref, block_ref, own_s):
    for y in range(8):
        own_s[160 * y : 160 * y + 160, :] = own_ref[y].astype(F32)

    def entries(first):
        rows = [own_s[pl.ds(first + s, 8, stride=160), :] for s in range(40)]
        return jnp.concatenate(rows, axis=1)

    m_re, m_im, a_re, a_im = [entries(40 * q) for q in range(4)]
    left_re = jnp.concatenate([m_re, m_im, a_re, a_im], axis=0).astype(BF16)
    left_im = jnp.concatenate([m_im, -m_re, a_im, -a_re], axis=0).astype(BF16)
    block = (mm_nt(left_re, p_ref[0]) + mm_nt(left_im, p_ref[1])) * (1.0 / 16384.0)
    shift = (128 - 2 * lax.axis_index("z")) % 128
    corr = block[:16, :24]
    corr = pltpu.roll(jnp.concatenate([corr, corr, jnp.zeros((16, 80), F32)], axis=1), shift, 1)
    row = [block[16:24, :24], block[24:, :24], corr[:8, :14], corr[8:, :14], jnp.zeros((8, 52), F32)]
    row = jnp.concatenate(row, axis=1)
    for peer in range(32):
        block_ref[peer] = row


def join_kernel(blocks_ref, joined_ref):
    sums = [(blocks_ref[y, 0] + blocks_ref[y, 1]) + (blocks_ref[y, 2] + blocks_ref[y, 3]) for y in range(8)]
    ham = [jnp.concatenate([sums[y][:, 24 * m : 24 * m + 24] for y in range(8)], axis=1) for m in range(2)]
    pad = [jnp.zeros((8, 16), F32)]
    corr = [
        jnp.concatenate([sums[y][:, 48 + 14 * m : 62 + 14 * m] for y in range(8)] + pad, axis=1) for m in range(2)
    ]
    tail = jnp.concatenate([ham[0][:, 128:], ham[1][:, 128:]], axis=1)
    joined = jnp.concatenate([ham[0][:, :128], ham[1][:, :128], tail] + corr, axis=0)
    for z in range(12):
        joined_ref[z] = joined


def corr_lanes():
    lane = np.arange(256)
    ahead = (lane % 24 - 2 * np.arange(12)[:, None]) % 24
    source = np.where((ahead < 14) & (lane < 192), lane // 24 * 14 + ahead, 0)
    return source.reshape(24, 128).astype(np.int32)


def last_kernel(all_ref, lane_ref, s_hbm, h_hbm, t_s, out_s, sems):
    for c in range(2):
        for z in range(12):
            rows = pl.ds(z * 2 + c, 8, stride=24)
            tail = all_ref[c, z, 16:24, :]
            t_s[0, rows, :] = all_ref[c, z, 0:8, :]
            t_s[1, rows, :] = tail
            t_s[2, rows, :] = all_ref[c, z, 8:16, :]
            t_s[3, rows, :] = jnp.concatenate([tail[:, 64:], tail[:, :64]], axis=1)
    sends = []
    for m in range(2):
        out_s[m, 0:128, :] = t_s[2 * m].T
        out_s[m, 128:192, :] = t_s[2 * m + 1].T[:64]
        sends.append(pltpu.make_async_copy(out_s.at[m], h_hbm.at[m], sems.at[m]))
        sends[-1].start()
    for z in range(12):
        low = jnp.broadcast_to(lane_ref[2 * z : 2 * z + 1, :], (8, 128))
        high = jnp.broadcast_to(lane_ref[2 * z + 1 : 2 * z + 2, :], (8, 128))
        for c in range(2):
            rows = pl.ds(z * 2 + c, 8, stride=24)
            for m in range(2):
                corr = all_ref[c, z, 24 + 8 * m : 32 + 8 * m, :]
                t_s[4 + 2 * m, rows, :] = jnp.take_along_axis(corr, low, axis=1)
                t_s[5 + 2 * m, rows, :] = jnp.take_along_axis(corr, high, axis=1)

    def z_of(band):
        return (band >> 1) - 12 * ((band * 2731) >> 16)

    for m in range(2):
        low, high = t_s[4 + 2 * m], t_s[5 + 2 * m]
        for start, count, turned in ((0, 128, low.T), (128, 64, high.T[:64])):
            band_i = lax.broadcasted_iota(jnp.int32, (count, 192), 0) + start
            band_j = lax.broadcasted_iota(jnp.int32, (count, 192), 1)
            ahead = z_of(band_i) - z_of(band_j)
            direct = ((ahead >= 0) & (ahead <= 6)) | (ahead <= -6)
            mirror = jnp.concatenate([low[start : start + count], high[start : start + count, :64]], axis=1)
            out_s[2 + m, start : start + count, :] = jnp.where(direct, turned, mirror if m == 0 else -mirror)
        sends.append(pltpu.make_async_copy(out_s.at[2 + m], s_hbm.at[m], sems.at[2 + m]))
        sends[-1].start()
    for send in sends:
        send.wait()


def call(kernel, outs, *args, scratch=(), **space):
    return pl.pallas_call(
        kernel,
        out_shape=outs,
        scratch_shapes=list(scratch),
        compiler_params=pltpu.CompilerParams(vmem_limit_bytes=48 * 1024 * 1024),
        **space,
    )(*args)


def shape(dims, dtype):
    return jax.ShapeDtypeStruct(dims, dtype)


def body(orbitals, potential, slot_sticks, stick_entries):
    wz, wx, bx, bz = tables(potential.shape[1], 64)
    own = orbitals.reshape(2, 40, 128)
    psi = lax.all_to_all(jnp.broadcast_to(own.reshape(80, 128), (12, 80, 128)), "z", 0, 0, tiled=True)
    packed = call(first_kernel, shape((560, 128), BF16), stick_entries, own, potential, bx)
    everyone = lax.all_gather(packed, "x")
    msg, out = call(
        main_kernel,
        [shape((8, 160, 128), BF16), shape((2, 40, 128), BF16)],
        everyone, own, stick_entries, slot_sticks.reshape(1, 160), slot_sticks.reshape(160, 1), wz, wx, bz,
    )
    arrived = lax.all_to_all(msg, "y", 0, 0, tiled=True)
    rows = call(
        rows_kernel, shape((2, 32, 5120), BF16), lax.all_gather(psi, "c"), scratch=[pltpu.VMEM((1920, 128), F32)]
    )
    block = call(product_kernel, shape((32, 8, 128), F32), rows, arrived, scratch=[pltpu.VMEM((1280, 128), F32)])
    blocks = lax.all_to_all(block, ("y", "x"), 0, 0, tiled=True)
    joined = call(join_kernel, shape((12, 40, 128), F32), blocks.reshape(8, 4, 8, 128))
    joined = lax.all_to_all(joined, "z", 0, 0, tiled=True)
    correlation, reduced = call(
        last_kernel,
        [shape((2, 192, 192), F32), shape((2, 192, 192), F32)],
        lax.all_gather(joined, "c"), corr_lanes(),
        scratch=[pltpu.VMEM((8, 192, 128), F32), pltpu.VMEM((4, 192, 192), F32), pltpu.SemaphoreType.DMA((4,))],
        out_specs=[pl.BlockSpec(memory_space=pltpu.HBM)] * 2,
    )
    return out.reshape(orbitals.shape), correlation, reduced


def solution(mesh):
    finer = Mesh(mesh.devices.reshape(8, 12, 2, mesh.shape["ga"]), ("y", "z", "c", "x"))
    return jax.shard_map(
        body,
        mesh=finer,
        in_specs=(P(None, BAND, "x", None), P("x", None), P(), P()),
        out_specs=(P(None, BAND, "x", None), P(), P()),
        check_vma=False,
    )
```

```python
import functools

import jax
import jax.numpy as jnp
import numpy as np
from jax import lax
from jax.experimental import pallas as pl
from jax.experimental.pallas import tpu as pltpu
from jax.sharding import Mesh
from jax.sharding import PartitionSpec as P

BAND = ("y", "z", "c")
M = 256
F32 = jnp.float32
BF16 = jnp.bfloat16

FIRST_Z, FIRST_Y, FIRST_YX, LAST_Z = 10, 2, (6, 2), 4


def turned(first, count):
    return [(first + k) % count for k in range(count)]


Z_ORDER, Y_ORDER, TAIL_ORDER = turned(FIRST_Z, 12), turned(FIRST_Y, 8), turned(LAST_Z, 12)
YX_ORDER = [4 * y + x for y in turned(FIRST_YX[0], 8) for x in turned(FIRST_YX[1], 4)]


def hi_lo(table):
    hi = table.astype(np.float32).astype(jnp.bfloat16)
    lo = (table - hi.astype(np.float64)).astype(np.float32).astype(jnp.bfloat16)
    return np.stack([hi, lo])


def tables(points, radius):
    freq = np.arange(2 * radius) - radius + 1
    pos = np.arange(M)
    ang = 2.0 * np.pi * ((freq[:, None] * pos[None, :]) % M) / M
    cos, sin = np.cos(ang), np.sin(ang)
    wz = np.block([[cos, sin], [-sin, cos]])
    top = 2 * radius - 2
    q = np.arange(1, top + 1)
    shift = pos[:, None] / M - np.arange(points)[None, :] / points
    resample = np.ones((M, points))
    for k in q:
        resample += 2.0 * np.cos(2.0 * np.pi * k * shift)
    resample /= points
    return hi_lo(wz), hi_lo(wz.T), hi_lo(resample.T), hi_lo(resample)


def split(x):
    hi = x.astype(BF16)
    return hi, (x - hi.astype(F32)).astype(BF16)


def mm(a, b):
    return lax.dot_general(a, b, (((1,), (0,)), ((), ())), preferred_element_type=F32)


def mm_nt(a, b):
    return lax.dot_general(a, b, (((1,), (1,)), ((), ())), preferred_element_type=F32)


def start_kernel(ent_hbm, orb_hbm, pot_hbm, zmsg_hbm, ent_ref, orb_ref, pot_ref, sems):
    first = pl.multiple_of(lax.axis_index("x") * 40, 8)
    pairs = [(orb_hbm, orb_ref), (ent_hbm.at[pl.ds(first, 40), :], ent_ref), (pot_hbm, pot_ref)]
    pairs += [(orb_ref, zmsg_hbm.at[z]) for z in range(12)]
    copies = [pltpu.make_async_copy(src, dst, sems.at[i]) for i, (src, dst) in enumerate(pairs)]
    for copy in copies[:3]:
        copy.start()
    copies[0].wait()
    for copy in copies[3:]:
        copy.start()
    for copy in copies[1:]:
        copy.wait()


def first_kernel(ent_ref, orb_ref, pot_ref, bx_ref, packed_ref):
    ent_t = ent_ref[...].T
    orb = orb_ref[...].astype(F32)
    lane = lax.broadcasted_iota(jnp.int32, (128, 128), 1)
    sub = lax.broadcasted_iota(jnp.int32, (128, 128), 0)
    pieces = [[], []]
    for g in range(5):
        rows = []
        for r in range(8):
            s = 8 * g + r
            match = ent_t[:, s : s + 1] == lane
            rows.append(jnp.max(jnp.where(match, sub, -1), axis=0, keepdims=True))
        source = jnp.concatenate(rows, axis=0)
        index = jnp.maximum(source, 0)
        for c in range(2):
            moved = jnp.take_along_axis(orb[c, 8 * g : 8 * g + 8, :], index, axis=1)
            pieces[c].append(jnp.where(source >= 0, moved, 0.0))
    spread = jnp.concatenate(pieces[0] + pieces[1], axis=0).astype(BF16)
    packed_ref[0:80, :] = spread
    v_hi, v_lo = split(pot_ref[...])
    vx = mm(v_hi, bx_ref[0]) + mm(v_lo, bx_ref[0]) + mm(v_hi, bx_ref[1])
    vx = jnp.concatenate([vx[:, :128], vx[:, 128:]], axis=0)
    hi, lo = split(vx)
    packed_ref[80:320, :] = hi
    packed_ref[320:560, :] = lo


def main_kernel(all_ref, orb_ref, ent_ref, slot_row_ref, slot_col_ref, wz_ref, wx_ref, bz_ref, msg_ref, out_ref):
    d = lax.axis_index("x")
    first = pl.multiple_of(d * 40, 8)

    def rows_of_all(start, count):
        return jnp.concatenate([all_ref[d, start : start + count, :].astype(F32) for d in range(4)], axis=0)

    def gathered_v(start):
        halves = [rows_of_all(start, 120), rows_of_all(start + 120, 120)]
        return jnp.concatenate(halves, axis=1).astype(BF16)

    v_hi = gathered_v(80)
    v_lo = gathered_v(320)
    pot = mm(bz_ref[0], v_hi) + mm(bz_ref[1], v_hi) + mm(bz_ref[0], v_lo)
    pot = pot.T

    place = (
        lax.broadcasted_iota(jnp.int32, (128, 160), 0) == jnp.broadcast_to(slot_row_ref[...], (128, 160))
    ).astype(F32).astype(BF16)
    c_re = rows_of_all(0, 40).astype(BF16)
    c_im = rows_of_all(40, 40).astype(BF16)
    sticks = jnp.concatenate([mm(place, c_re), mm(place, c_im)], axis=0).astype(BF16)

    t = mm(wx_ref[0], sticks) + mm(wx_ref[1], sticks)
    t = jnp.concatenate([t[:M], t[M:]], axis=1)
    t_hi, t_lo = split(t)
    field = mm(t_hi, wz_ref[0]) + mm(t_lo, wz_ref[0]) + mm(t_hi, wz_ref[1])
    prod = jnp.concatenate([field[:, :M] * pot, field[:, M:] * pot], axis=1)
    p_hi, p_lo = split(prod)
    y = mm(p_hi, wx_ref[0]) + mm(p_lo, wx_ref[0]) + mm(p_hi, wx_ref[1])
    y = jnp.concatenate([y[:, :128], y[:, 128:]], axis=0)
    y_hi, y_lo = split(y)

    slot = slot_col_ref[pl.ds(first, 40), :]
    pick = (lax.broadcasted_iota(jnp.int32, (40, 128), 1) == slot).astype(F32)
    none = jnp.zeros((40, 128), F32)
    pick = jnp.concatenate(
        [jnp.concatenate([pick, none], axis=1), jnp.concatenate([none, pick], axis=1)], axis=0
    ).astype(BF16)
    w_hi = mm(pick, wz_ref[0]).astype(BF16)
    w_lo = mm(pick, wz_ref[1]).astype(BF16)
    applied = (mm(w_hi, y_hi) + mm(w_hi, y_lo) + mm(w_lo, y_hi)) * (1.0 / (M * M))

    gx = slot - 63
    gz = lax.broadcasted_iota(jnp.int32, (40, 128), 1) - 63
    square = gx * gx + gz * gz
    inside = (square < 64 * 64) & (slot >= 0)
    kinetic = square.astype(F32) * (1.0 / 4096.0)
    own = all_ref[d, 0:80, :].astype(F32)
    ent = ent_ref[...]
    index = jnp.maximum(ent, 0)
    masked, applied_rows = [], []
    for c in range(2):
        value = kinetic * own[40 * c : 40 * c + 40] + applied[40 * c : 40 * c + 40]
        h = jnp.where(inside, value, 0.0).astype(BF16).astype(F32)
        moved = [jnp.take_along_axis(h[8 * g : 8 * g + 8], index[8 * g : 8 * g + 8], axis=1) for g in range(5)]
        applied_rows.append(jnp.where(ent >= 0, jnp.concatenate(moved, axis=0), 0.0))
        masked.append(jnp.where(ent >= 0, orb_ref[c].astype(F32), 0.0))
        out_ref[c] = applied_rows[c].astype(BF16)
    message = jnp.concatenate(masked + applied_rows, axis=0).astype(BF16)
    for y in range(8):
        msg_ref[y] = message


def rows_kernel(psi_ref, p_ref, psi_s):
    for c in range(2):
        for k, z in enumerate(Z_ORDER):
            at = (2 * z + c) * 80
            for part in range(2):
                psi_s[at + 40 * part : at + 40 * part + 40, :] = psi_ref[c, k, part].astype(F32)
    pad = jnp.zeros((8, 128), F32)
    for part in range(2):
        for s in range(40):
            block = jnp.concatenate([psi_s[pl.ds(40 * part + s, 24, stride=80), :], pad], axis=0)
            p_ref[part, :, 128 * s : 128 * s + 128] = block.astype(BF16)


def product_kernel(p_ref, own_ref, block_ref, own_s):
    for k, y in enumerate(Y_ORDER):
        own_s[160 * y : 160 * y + 160, :] = own_ref[k].astype(F32)

    def entries(first):
        rows = [own_s[pl.ds(first + s, 8, stride=160), :] for s in range(40)]
        return jnp.concatenate(rows, axis=1)

    m_re, m_im, a_re, a_im = [entries(40 * q) for q in range(4)]
    left_re = jnp.concatenate([m_re, m_im, a_re, a_im], axis=0).astype(BF16)
    left_im = jnp.concatenate([m_im, -m_re, a_im, -a_re], axis=0).astype(BF16)
    block = (mm_nt(left_re, p_ref[0]) + mm_nt(left_im, p_ref[1])) * (1.0 / 16384.0)
    shift = (128 - 2 * lax.axis_index("z")) % 128
    corr = block[:16, :24]
    corr = pltpu.roll(jnp.concatenate([corr, corr, jnp.zeros((16, 80), F32)], axis=1), shift, 1)
    row = [block[16:24, :24], block[24:, :24], corr[:8, :14], corr[8:, :14], jnp.zeros((8, 52), F32)]
    row = jnp.concatenate(row, axis=1)
    for peer in range(32):
        block_ref[peer] = row


def join_kernel(blocks_ref, joined_ref):
    def part(y, x):
        return blocks_ref[YX_ORDER.index(4 * y + x)]

    sums = [(part(y, 0) + part(y, 1)) + (part(y, 2) + part(y, 3)) for y in range(8)]
    ham = [jnp.concatenate([sums[y][:, 24 * m : 24 * m + 24] for y in range(8)], axis=1) for m in range(2)]
    pad = [jnp.zeros((8, 16), F32)]
    corr = [
        jnp.concatenate([sums[y][:, 48 + 14 * m : 62 + 14 * m] for y in range(8)] + pad, axis=1) for m in range(2)
    ]
    tail = jnp.concatenate([ham[0][:, 128:], ham[1][:, 128:]], axis=1)
    joined = jnp.concatenate([ham[0][:, :128], ham[1][:, :128], tail] + corr, axis=0)
    for z in range(12):
        joined_ref[z] = joined


def corr_lanes():
    lane = np.arange(256)
    ahead = (lane % 24 - 2 * np.arange(12)[:, None]) % 24
    source = np.where((ahead < 14) & (lane < 192), lane // 24 * 14 + ahead, 0)
    return source.reshape(24, 128).astype(np.int32)


def last_kernel(all_ref, lane_ref, s_hbm, h_hbm, t_s, out_s, sems):
    for c in range(2):
        for k, z in enumerate(TAIL_ORDER):
            rows = pl.ds(z * 2 + c, 8, stride=24)
            tail = all_ref[c, k, 16:24, :]
            t_s[0, rows, :] = all_ref[c, k, 0:8, :]
            t_s[1, rows, :] = tail
            t_s[2, rows, :] = all_ref[c, k, 8:16, :]
            t_s[3, rows, :] = jnp.concatenate([tail[:, 64:], tail[:, :64]], axis=1)
    sends = []
    for m in range(2):
        out_s[m, 0:128, :] = t_s[2 * m].T
        out_s[m, 128:192, :] = t_s[2 * m + 1].T[:64]
        sends.append(pltpu.make_async_copy(out_s.at[m], h_hbm.at[m], sems.at[m]))
        sends[-1].start()
    for k, z in enumerate(TAIL_ORDER):
        low = jnp.broadcast_to(lane_ref[2 * z : 2 * z + 1, :], (8, 128))
        high = jnp.broadcast_to(lane_ref[2 * z + 1 : 2 * z + 2, :], (8, 128))
        for c in range(2):
            rows = pl.ds(z * 2 + c, 8, stride=24)
            for m in range(2):
                corr = all_ref[c, k, 24 + 8 * m : 32 + 8 * m, :]
                t_s[4 + 2 * m, rows, :] = jnp.take_along_axis(corr, low, axis=1)
                t_s[5 + 2 * m, rows, :] = jnp.take_along_axis(corr, high, axis=1)

    def z_of(band):
        return (band >> 1) - 12 * ((band * 2731) >> 16)

    for m in range(2):
        low, high = t_s[4 + 2 * m], t_s[5 + 2 * m]
        for start, count, turned in ((0, 128, low.T), (128, 64, high.T[:64])):
            band_i = lax.broadcasted_iota(jnp.int32, (count, 192), 0) + start
            band_j = lax.broadcasted_iota(jnp.int32, (count, 192), 1)
            ahead = z_of(band_i) - z_of(band_j)
            direct = ((ahead >= 0) & (ahead <= 6)) | (ahead <= -6)
            mirror = jnp.concatenate([low[start : start + count], high[start : start + count, :64]], axis=1)
            out_s[2 + m, start : start + count, :] = jnp.where(direct, turned, mirror if m == 0 else -mirror)
        sends.append(pltpu.make_async_copy(out_s.at[2 + m], s_hbm.at[m], sems.at[2 + m]))
        sends[-1].start()
    for send in sends:
        send.wait()


def call(kernel, outs, *args, scratch=(), **space):
    return pl.pallas_call(
        kernel,
        out_shape=outs,
        scratch_shapes=list(scratch),
        compiler_params=pltpu.CompilerParams(vmem_limit_bytes=48 * 1024 * 1024),
        **space,
    )(*args)


def shape(dims, dtype):
    return jax.ShapeDtypeStruct(dims, dtype)


def exchange(array, axis, order):
    return lax.all_to_all(array, axis, 0, 0, tiled=True, axis_index_groups=[order])


def body(orbitals, potential, slot_sticks, stick_entries):
    wz, wx, bx, bz = tables(potential.shape[1], 64)
    args = [stick_entries, orbitals.reshape(2, 40, 128), potential]
    zmsg, ent, own, pot = call(
        start_kernel,
        [shape((12, 2, 40, 128), BF16), shape((40, 128), jnp.int32), shape((2, 40, 128), BF16), shape((120, 480), F32)],
        *[pltpu.with_memory_space_constraint(a, pltpu.HBM) for a in args],
        scratch=[pltpu.SemaphoreType.DMA((15,))],
        in_specs=[pl.BlockSpec(memory_space=pltpu.HBM)] * 3,
        out_specs=[pl.BlockSpec(memory_space=pltpu.HBM)] + [pl.BlockSpec(memory_space=pltpu.VMEM)] * 3,
    )
    psi = exchange(zmsg, "z", Z_ORDER)
    packed = call(first_kernel, shape((560, 128), BF16), ent, own, pot, bx)
    everyone = lax.all_gather(packed, "x")
    msg, out = call(
        main_kernel,
        [shape((8, 160, 128), BF16), shape((2, 40, 128), BF16)],
        everyone, own, ent, slot_sticks.reshape(1, 160), slot_sticks.reshape(160, 1), wz, wx, bz,
    )
    arrived = exchange(msg, "y", Y_ORDER)
    rows = call(
        rows_kernel, shape((2, 32, 5120), BF16), lax.all_gather(psi, "c"), scratch=[pltpu.VMEM((1920, 128), F32)]
    )
    block = call(product_kernel, shape((32, 8, 128), F32), rows, arrived, scratch=[pltpu.VMEM((1280, 128), F32)])
    blocks = exchange(block, ("y", "x"), YX_ORDER)
    joined = call(join_kernel, shape((12, 40, 128), F32), blocks)
    joined = exchange(joined, "z", TAIL_ORDER)
    correlation, reduced = call(
        last_kernel,
        [shape((2, 192, 192), F32), shape((2, 192, 192), F32)],
        lax.all_gather(joined, "c"), corr_lanes(),
        scratch=[pltpu.VMEM((8, 192, 128), F32), pltpu.VMEM((4, 192, 192), F32), pltpu.SemaphoreType.DMA((4,))],
        out_specs=[pl.BlockSpec(memory_space=pltpu.HBM)] * 2,
    )
    return out.reshape(orbitals.shape), correlation, reduced


def solution(mesh):
    finer = Mesh(mesh.devices.reshape(8, 12, 2, mesh.shape["ga"]), ("y", "z", "c", "x"))
    return jax.shard_map(
        body,
        mesh=finer,
        in_specs=(P(None, BAND, "x", None), P("x", None), P(), P()),
        out_specs=(P(None, BAND, "x", None), P(), P()),
        check_vma=False,
    )
```

```python
import functools

import jax
import jax.numpy as jnp
import numpy as np
from jax import lax
from jax.experimental import pallas as pl
from jax.experimental.pallas import tpu as pltpu
from jax.sharding import Mesh
from jax.sharding import PartitionSpec as P

BAND = ("y", "z", "c")
M = 256
F32 = jnp.float32
BF16 = jnp.bfloat16

FIRST_Z, FIRST_Y, FIRST_YX, LAST_Z = 11, 3, (7, 2), 5


def turned(first, count):
    return [(first + k) % count for k in range(count)]


Z_ORDER, Y_ORDER, TAIL_ORDER = turned(FIRST_Z, 12), turned(FIRST_Y, 8), turned(LAST_Z, 12)
YX_ORDER = [4 * y + x for y in turned(FIRST_YX[0], 8) for x in turned(FIRST_YX[1], 4)]


def hi_lo(table):
    hi = table.astype(np.float32).astype(jnp.bfloat16)
    lo = (table - hi.astype(np.float64)).astype(np.float32).astype(jnp.bfloat16)
    return np.stack([hi, lo])


def tables(points, radius):
    freq = np.arange(2 * radius) - radius + 1
    pos = np.arange(M)
    ang = 2.0 * np.pi * ((freq[:, None] * pos[None, :]) % M) / M
    cos, sin = np.cos(ang), np.sin(ang)
    wz = np.block([[cos, sin], [-sin, cos]])
    top = 2 * radius - 2
    q = np.arange(1, top + 1)
    shift = pos[:, None] / M - np.arange(points)[None, :] / points
    resample = np.ones((M, points))
    for k in q:
        resample += 2.0 * np.cos(2.0 * np.pi * k * shift)
    resample /= points
    return hi_lo(wz), hi_lo(wz.T), hi_lo(resample.T), hi_lo(resample)


def split(x):
    hi = x.astype(BF16)
    return hi, (x - hi.astype(F32)).astype(BF16)


def mm(a, b):
    return lax.dot_general(a, b, (((1,), (0,)), ((), ())), preferred_element_type=F32)


def mm_nt(a, b):
    return lax.dot_general(a, b, (((1,), (1,)), ((), ())), preferred_element_type=F32)


def start_kernel(
    ent_hbm, orb_hbm, pot_hbm, slot_hbm, zmsg_hbm, ent_ref, orb_ref, pot_ref, slot_ref, sems
):
    first = pl.multiple_of(lax.axis_index("x") * 40, 8)
    pairs = [(orb_hbm, orb_ref), (ent_hbm.at[pl.ds(first, 40), :], ent_ref), (pot_hbm, pot_ref)]
    pairs.append((slot_hbm, slot_ref))
    pairs += [(orb_ref, zmsg_hbm.at[z]) for z in range(12)]
    copies = [pltpu.make_async_copy(src, dst, sems.at[i]) for i, (src, dst) in enumerate(pairs)]
    for copy in copies[:4]:
        copy.start()
    copies[0].wait()
    for copy in copies[4:]:
        copy.start()
    for copy in copies[1:]:
        copy.wait()


def first_kernel(ent_ref, orb_ref, pot_ref, bx_ref, packed_ref):
    ent_t = ent_ref[...].T
    orb = orb_ref[...].astype(F32)
    lane = lax.broadcasted_iota(jnp.int32, (128, 128), 1)
    sub = lax.broadcasted_iota(jnp.int32, (128, 128), 0)
    pieces = [[], []]
    for g in range(5):
        rows = []
        for r in range(8):
            s = 8 * g + r
            match = ent_t[:, s : s + 1] == lane
            rows.append(jnp.max(jnp.where(match, sub, -1), axis=0, keepdims=True))
        source = jnp.concatenate(rows, axis=0)
        index = jnp.maximum(source, 0)
        for c in range(2):
            moved = jnp.take_along_axis(orb[c, 8 * g : 8 * g + 8, :], index, axis=1)
            pieces[c].append(jnp.where(source >= 0, moved, 0.0))
    spread = jnp.concatenate(pieces[0] + pieces[1], axis=0).astype(BF16)
    packed_ref[0:80, :] = spread
    v_hi, v_lo = split(pot_ref[...])
    vx = mm(v_hi, bx_ref[0]) + mm(v_lo, bx_ref[0]) + mm(v_hi, bx_ref[1])
    vx = jnp.concatenate([vx[:, :128], vx[:, 128:]], axis=0)
    hi, lo = split(vx)
    packed_ref[80:320, :] = hi
    packed_ref[320:560, :] = lo


def main_kernel(all_ref, orb_ref, ent_ref, slot_row_ref, slot_col_ref, wz_ref, wx_ref, bz_ref, msg_ref, out_ref):
    d = lax.axis_index("x")
    first = pl.multiple_of(d * 40, 8)

    def rows_of_all(start, count):
        return jnp.concatenate([all_ref[k, start : start + count, :].astype(F32) for k in range(4)], axis=0)

    def gathered_v(start):
        halves = [rows_of_all(start, 120), rows_of_all(start + 120, 120)]
        return jnp.concatenate(halves, axis=1).astype(BF16)

    v_hi = gathered_v(80)
    v_lo = gathered_v(320)
    pot = mm(bz_ref[0], v_hi) + mm(bz_ref[1], v_hi) + mm(bz_ref[0], v_lo)
    pot = pot.T

    place = (
        lax.broadcasted_iota(jnp.int32, (128, 160), 0) == jnp.broadcast_to(slot_row_ref[...], (128, 160))
    ).astype(F32).astype(BF16)
    c_re = rows_of_all(0, 40).astype(BF16)
    c_im = rows_of_all(40, 40).astype(BF16)
    sticks = jnp.concatenate([mm(place, c_re), mm(place, c_im)], axis=0).astype(BF16)

    t = mm(wx_ref[0], sticks) + mm(wx_ref[1], sticks)
    t = jnp.concatenate([t[:M], t[M:]], axis=1)
    t_hi, t_lo = split(t)
    field = mm(t_hi, wz_ref[0]) + mm(t_lo, wz_ref[0]) + mm(t_hi, wz_ref[1])
    prod = jnp.concatenate([field[:, :M] * pot, field[:, M:] * pot], axis=1)
    p_hi, p_lo = split(prod)
    y = mm(p_hi, wx_ref[0]) + mm(p_lo, wx_ref[0]) + mm(p_hi, wx_ref[1])
    y = jnp.concatenate([y[:, :128], y[:, 128:]], axis=0)
    y_hi, y_lo = split(y)

    slot = slot_col_ref[pl.ds(first, 40), :]
    pick = (lax.broadcasted_iota(jnp.int32, (40, 128), 1) == slot).astype(F32)
    none = jnp.zeros((40, 128), F32)
    pick = jnp.concatenate(
        [jnp.concatenate([pick, none], axis=1), jnp.concatenate([none, pick], axis=1)], axis=0
    ).astype(BF16)
    w_hi = mm(pick, wz_ref[0]).astype(BF16)
    w_lo = mm(pick, wz_ref[1]).astype(BF16)
    applied = (mm(w_hi, y_hi) + mm(w_hi, y_lo) + mm(w_lo, y_hi)) * (1.0 / (M * M))

    gx = slot - 63
    gz = lax.broadcasted_iota(jnp.int32, (40, 128), 1) - 63
    square = gx * gx + gz * gz
    inside = (square < 64 * 64) & (slot >= 0)
    kinetic = square.astype(F32) * (1.0 / 4096.0)
    own = all_ref[d, 0:80, :].astype(F32)
    ent = ent_ref[...]
    index = jnp.maximum(ent, 0)
    masked, applied_rows = [], []
    for c in range(2):
        value = kinetic * own[40 * c : 40 * c + 40] + applied[40 * c : 40 * c + 40]
        h = jnp.where(inside, value, 0.0).astype(BF16).astype(F32)
        moved = [jnp.take_along_axis(h[8 * g : 8 * g + 8], index[8 * g : 8 * g + 8], axis=1) for g in range(5)]
        applied_rows.append(jnp.where(ent >= 0, jnp.concatenate(moved, axis=0), 0.0))
        masked.append(jnp.where(ent >= 0, orb_ref[c].astype(F32), 0.0))
        out_ref[c] = applied_rows[c].astype(BF16)
    message = jnp.concatenate(masked + applied_rows, axis=0).astype(BF16)
    for y in range(8):
        msg_ref[y] = message


def rows_kernel(psi_ref, p_ref, psi_s):
    for c in range(2):
        for k, z in enumerate(Z_ORDER):
            at = (2 * z + c) * 80
            for part in range(2):
                psi_s[at + 40 * part : at + 40 * part + 40, :] = psi_ref[c, k, part].astype(F32)
    pad = jnp.zeros((8, 128), F32)
    for part in range(2):
        for s in range(40):
            block = jnp.concatenate([psi_s[pl.ds(40 * part + s, 24, stride=80), :], pad], axis=0)
            p_ref[part, :, 128 * s : 128 * s + 128] = block.astype(BF16)


def product_kernel(p_ref, own_ref, block_ref, own_s):
    for k, y in enumerate(Y_ORDER):
        own_s[160 * y : 160 * y + 160, :] = own_ref[k].astype(F32)

    def entries(first):
        rows = [own_s[pl.ds(first + s, 8, stride=160), :] for s in range(40)]
        return jnp.concatenate(rows, axis=1)

    m_re, m_im, a_re, a_im = [entries(40 * q) for q in range(4)]
    left_re = jnp.concatenate([m_re, m_im, a_re, a_im], axis=0).astype(BF16)
    left_im = jnp.concatenate([m_im, -m_re, a_im, -a_re], axis=0).astype(BF16)
    block = (mm_nt(left_re, p_ref[0]) + mm_nt(left_im, p_ref[1])) * (1.0 / 16384.0)
    shift = (128 - 2 * lax.axis_index("z")) % 128
    corr = block[:16, :24]
    corr = pltpu.roll(jnp.concatenate([corr, corr, jnp.zeros((16, 80), F32)], axis=1), shift, 1)
    row = [block[16:24, :24], block[24:, :24], corr[:8, :14], corr[8:, :14], jnp.zeros((8, 52), F32)]
    row = jnp.concatenate(row, axis=1)
    for peer in range(32):
        block_ref[peer] = row


def join_kernel(blocks_ref, joined_ref):
    def part(y, x):
        return blocks_ref[YX_ORDER.index(4 * y + x)]

    sums = [(part(y, 0) + part(y, 1)) + (part(y, 2) + part(y, 3)) for y in range(8)]
    ham = [jnp.concatenate([sums[y][:, 24 * m : 24 * m + 24] for y in range(8)], axis=1) for m in range(2)]
    pad = [jnp.zeros((8, 16), F32)]
    corr = [
        jnp.concatenate([sums[y][:, 48 + 14 * m : 62 + 14 * m] for y in range(8)] + pad, axis=1) for m in range(2)
    ]
    tail = jnp.concatenate([ham[0][:, 128:], ham[1][:, 128:]], axis=1)
    joined = jnp.concatenate([ham[0][:, :128], ham[1][:, :128], tail] + corr, axis=0)
    for z in range(12):
        joined_ref[z] = joined


def corr_lanes():
    lane = np.arange(256)
    ahead = (lane % 24 - 2 * np.arange(12)[:, None]) % 24
    source = np.where((ahead < 14) & (lane < 192), lane // 24 * 14 + ahead, 0)
    return source.reshape(24, 128).astype(np.int32)


def last_kernel(all_ref, lane_ref, s_hbm, h_hbm, t_s, out_s, sems):
    for c in range(2):
        for k, z in enumerate(TAIL_ORDER):
            rows = pl.ds(z * 2 + c, 8, stride=24)
            tail = all_ref[c, k, 16:24, :]
            t_s[0, rows, :] = all_ref[c, k, 0:8, :]
            t_s[1, rows, :] = tail
            t_s[2, rows, :] = all_ref[c, k, 8:16, :]
            t_s[3, rows, :] = jnp.concatenate([tail[:, 64:], tail[:, :64]], axis=1)
    sends = []
    for m in range(2):
        out_s[m, 0:128, :] = t_s[2 * m].T
        out_s[m, 128:192, :] = t_s[2 * m + 1].T[:64]
        sends.append(pltpu.make_async_copy(out_s.at[m], h_hbm.at[m], sems.at[m]))
        sends[-1].start()
    for k, z in enumerate(TAIL_ORDER):
        low = jnp.broadcast_to(lane_ref[2 * z : 2 * z + 1, :], (8, 128))
        high = jnp.broadcast_to(lane_ref[2 * z + 1 : 2 * z + 2, :], (8, 128))
        for c in range(2):
            rows = pl.ds(z * 2 + c, 8, stride=24)
            for m in range(2):
                corr = all_ref[c, k, 24 + 8 * m : 32 + 8 * m, :]
                t_s[4 + 2 * m, rows, :] = jnp.take_along_axis(corr, low, axis=1)
                t_s[5 + 2 * m, rows, :] = jnp.take_along_axis(corr, high, axis=1)

    def z_of(band):
        return (band >> 1) - 12 * ((band * 2731) >> 16)

    for m in range(2):
        low, high = t_s[4 + 2 * m], t_s[5 + 2 * m]
        for start, count, turned in ((0, 128, low.T), (128, 64, high.T[:64])):
            band_i = lax.broadcasted_iota(jnp.int32, (count, 192), 0) + start
            band_j = lax.broadcasted_iota(jnp.int32, (count, 192), 1)
            ahead = z_of(band_i) - z_of(band_j)
            direct = ((ahead >= 0) & (ahead <= 6)) | (ahead <= -6)
            mirror = jnp.concatenate([low[start : start + count], high[start : start + count, :64]], axis=1)
            out_s[2 + m, start : start + count, :] = jnp.where(direct, turned, mirror if m == 0 else -mirror)
        sends.append(pltpu.make_async_copy(out_s.at[2 + m], s_hbm.at[m], sems.at[2 + m]))
        sends[-1].start()
    for send in sends:
        send.wait()


def call(kernel, outs, *args, scratch=(), **space):
    return pl.pallas_call(
        kernel,
        out_shape=outs,
        scratch_shapes=list(scratch),
        compiler_params=pltpu.CompilerParams(vmem_limit_bytes=48 * 1024 * 1024),
        **space,
    )(*args)


def shape(dims, dtype):
    return jax.ShapeDtypeStruct(dims, dtype)


def exchange(array, axis, order):
    return lax.all_to_all(array, axis, 0, 0, tiled=True, axis_index_groups=[order])


def body(orbitals, potential, slot_sticks, stick_entries):
    wz, wx, bx, bz = tables(potential.shape[1], 64)
    args = [stick_entries, orbitals.reshape(2, 40, 128), potential, slot_sticks.reshape(1, 160)]
    zmsg, ent, own, pot, slots = call(
        start_kernel,
        [
            shape((12, 2, 40, 128), BF16),
            shape((40, 128), jnp.int32),
            shape((2, 40, 128), BF16),
            shape((120, 480), F32),
            shape((1, 160), jnp.int32),
        ],
        *[pltpu.with_memory_space_constraint(a, pltpu.HBM) for a in args],
        scratch=[pltpu.SemaphoreType.DMA((16,))],
        in_specs=[pl.BlockSpec(memory_space=pltpu.HBM)] * 4,
        out_specs=[pl.BlockSpec(memory_space=pltpu.HBM)] + [pl.BlockSpec(memory_space=pltpu.VMEM)] * 4,
    )
    psi = exchange(zmsg, "z", Z_ORDER)
    packed = call(first_kernel, shape((560, 128), BF16), ent, own, pot, bx)
    everyone = lax.all_gather(packed, "x")
    msg, out = call(
        main_kernel,
        [shape((8, 160, 128), BF16), shape((2, 40, 128), BF16)],
        everyone, own, ent, slots, slots.reshape(160, 1), wz, wx, bz,
    )
    arrived = exchange(msg, "y", Y_ORDER)
    rows = call(
        rows_kernel, shape((2, 32, 5120), BF16), lax.all_gather(psi, "c"), scratch=[pltpu.VMEM((1920, 128), F32)]
    )
    block = call(product_kernel, shape((32, 8, 128), F32), rows, arrived, scratch=[pltpu.VMEM((1280, 128), F32)])
    blocks = exchange(block, ("y", "x"), YX_ORDER)
    joined = call(join_kernel, shape((12, 40, 128), F32), blocks)
    joined = exchange(joined, "z", TAIL_ORDER)
    correlation, reduced = call(
        last_kernel,
        [shape((2, 192, 192), F32), shape((2, 192, 192), F32)],
        lax.all_gather(joined, "c"), corr_lanes(),
        scratch=[pltpu.VMEM((8, 192, 128), F32), pltpu.VMEM((4, 192, 192), F32), pltpu.SemaphoreType.DMA((4,))],
        out_specs=[pl.BlockSpec(memory_space=pltpu.HBM)] * 2,
    )
    return out.reshape(orbitals.shape), correlation, reduced


def solution(mesh):
    finer = Mesh(mesh.devices.reshape(8, 12, 2, mesh.shape["ga"]), ("y", "z", "c", "x"))
    return jax.shard_map(
        body,
        mesh=finer,
        in_specs=(P(None, BAND, "x", None), P("x", None), P(), P()),
        out_specs=(P(None, BAND, "x", None), P(), P()),
        check_vma=False,
    )
```

```python
import functools

import jax
import jax.numpy as jnp
import numpy as np
from jax import lax
from jax.experimental import pallas as pl
from jax.experimental.pallas import tpu as pltpu
from jax.sharding import Mesh
from jax.sharding import PartitionSpec as P

BAND = ("y", "z", "c")
M = 256
F32 = jnp.float32
BF16 = jnp.bfloat16

FIRST_Z, FIRST_Y, FIRST_YX, LAST_Z = 11, 3, (3, 2), 5


def turned(first, count):
    return [(first + k) % count for k in range(count)]


def outward(first, count):
    return [(first + (k + 1) // 2 * (1 if k % 2 else -1)) % count for k in range(count)]


Z_ORDER, Y_ORDER, TAIL_ORDER = turned(FIRST_Z, 12), outward(FIRST_Y, 8), outward(LAST_Z, 12)
YX_ORDER = [4 * y + x for y in turned(FIRST_YX[0], 8) for x in turned(FIRST_YX[1], 4)]


def hi_lo(table):
    hi = table.astype(np.float32).astype(jnp.bfloat16)
    lo = (table - hi.astype(np.float64)).astype(np.float32).astype(jnp.bfloat16)
    return np.stack([hi, lo])


def tables(points, radius):
    freq = np.arange(2 * radius) - radius + 1
    pos = np.arange(M)
    ang = 2.0 * np.pi * ((freq[:, None] * pos[None, :]) % M) / M
    cos, sin = np.cos(ang), np.sin(ang)
    wz = np.block([[cos, sin], [-sin, cos]])
    top = 2 * radius - 2
    q = np.arange(1, top + 1)
    shift = pos[:, None] / M - np.arange(points)[None, :] / points
    resample = np.ones((M, points))
    for k in q:
        resample += 2.0 * np.cos(2.0 * np.pi * k * shift)
    resample /= points
    return hi_lo(wz), hi_lo(wz.T), hi_lo(resample.T), hi_lo(resample)


def split(x):
    hi = x.astype(BF16)
    return hi, (x - hi.astype(F32)).astype(BF16)


def mm(a, b):
    return lax.dot_general(a, b, (((1,), (0,)), ((), ())), preferred_element_type=F32)


def mm_nt(a, b):
    return lax.dot_general(a, b, (((1,), (1,)), ((), ())), preferred_element_type=F32)


def start_kernel(
    ent_hbm, orb_hbm, pot_hbm, slot_hbm, zmsg_hbm, ent_ref, orb_ref, pot_ref, slot_ref, sems
):
    first = pl.multiple_of(lax.axis_index("x") * 40, 8)
    pairs = [(orb_hbm, orb_ref), (ent_hbm.at[pl.ds(first, 40), :], ent_ref), (pot_hbm, pot_ref)]
    pairs.append((slot_hbm, slot_ref))
    pairs += [(orb_ref, zmsg_hbm.at[z]) for z in range(12)]
    copies = [pltpu.make_async_copy(src, dst, sems.at[i]) for i, (src, dst) in enumerate(pairs)]
    for copy in copies[:4]:
        copy.start()
    copies[0].wait()
    for copy in copies[4:]:
        copy.start()
    for copy in copies[1:]:
        copy.wait()


def first_kernel(ent_ref, orb_ref, pot_ref, bx_ref, packed_ref):
    ent_t = ent_ref[...].T
    orb = orb_ref[...].astype(F32)
    lane = lax.broadcasted_iota(jnp.int32, (128, 128), 1)
    sub = lax.broadcasted_iota(jnp.int32, (128, 128), 0)
    pieces = [[], []]
    for g in range(5):
        rows = []
        for r in range(8):
            s = 8 * g + r
            match = ent_t[:, s : s + 1] == lane
            rows.append(jnp.max(jnp.where(match, sub, -1), axis=0, keepdims=True))
        source = jnp.concatenate(rows, axis=0)
        index = jnp.maximum(source, 0)
        for c in range(2):
            moved = jnp.take_along_axis(orb[c, 8 * g : 8 * g + 8, :], index, axis=1)
            pieces[c].append(jnp.where(source >= 0, moved, 0.0))
    spread = jnp.concatenate(pieces[0] + pieces[1], axis=0).astype(BF16)
    packed_ref[0:80, :] = spread
    v_hi, v_lo = split(pot_ref[...])
    vx = mm(v_hi, bx_ref[0]) + mm(v_lo, bx_ref[0]) + mm(v_hi, bx_ref[1])
    vx = jnp.concatenate([vx[:, :128], vx[:, 128:]], axis=0)
    hi, lo = split(vx)
    packed_ref[80:320, :] = hi
    packed_ref[320:560, :] = lo


def main_kernel(all_ref, orb_ref, ent_ref, slot_row_ref, slot_col_ref, wz_ref, wx_ref, bz_ref, msg_ref, out_ref):
    d = lax.axis_index("x")
    first = pl.multiple_of(d * 40, 8)

    def rows_of_all(start, count):
        return jnp.concatenate([all_ref[k, start : start + count, :].astype(F32) for k in range(4)], axis=0)

    def gathered_v(start):
        halves = [rows_of_all(start, 120), rows_of_all(start + 120, 120)]
        return jnp.concatenate(halves, axis=1).astype(BF16)

    v_hi = gathered_v(80)
    v_lo = gathered_v(320)
    pot = mm(bz_ref[0], v_hi) + mm(bz_ref[1], v_hi) + mm(bz_ref[0], v_lo)
    pot = pot.T

    place = (
        lax.broadcasted_iota(jnp.int32, (128, 160), 0) == jnp.broadcast_to(slot_row_ref[...], (128, 160))
    ).astype(F32).astype(BF16)
    c_re = rows_of_all(0, 40).astype(BF16)
    c_im = rows_of_all(40, 40).astype(BF16)
    sticks = jnp.concatenate([mm(place, c_re), mm(place, c_im)], axis=0).astype(BF16)

    t = mm(wx_ref[0], sticks) + mm(wx_ref[1], sticks)
    t = jnp.concatenate([t[:M], t[M:]], axis=1)
    t_hi, t_lo = split(t)
    field = mm(t_hi, wz_ref[0]) + mm(t_lo, wz_ref[0]) + mm(t_hi, wz_ref[1])
    prod = jnp.concatenate([field[:, :M] * pot, field[:, M:] * pot], axis=1)
    p_hi, p_lo = split(prod)
    y = mm(p_hi, wx_ref[0]) + mm(p_lo, wx_ref[0]) + mm(p_hi, wx_ref[1])
    y = jnp.concatenate([y[:, :128], y[:, 128:]], axis=0)
    y_hi, y_lo = split(y)

    slot = slot_col_ref[pl.ds(first, 40), :]
    pick = (lax.broadcasted_iota(jnp.int32, (40, 128), 1) == slot).astype(F32)
    none = jnp.zeros((40, 128), F32)
    pick = jnp.concatenate(
        [jnp.concatenate([pick, none], axis=1), jnp.concatenate([none, pick], axis=1)], axis=0
    ).astype(BF16)
    w_hi = mm(pick, wz_ref[0]).astype(BF16)
    w_lo = mm(pick, wz_ref[1]).astype(BF16)
    applied = (mm(w_hi, y_hi) + mm(w_hi, y_lo) + mm(w_lo, y_hi)) * (1.0 / (M * M))

    gx = slot - 63
    gz = lax.broadcasted_iota(jnp.int32, (40, 128), 1) - 63
    square = gx * gx + gz * gz
    inside = (square < 64 * 64) & (slot >= 0)
    kinetic = square.astype(F32) * (1.0 / 4096.0)
    own = all_ref[d, 0:80, :].astype(F32)
    ent = ent_ref[...]
    index = jnp.maximum(ent, 0)
    masked, applied_rows = [], []
    for c in range(2):
        value = kinetic * own[40 * c : 40 * c + 40] + applied[40 * c : 40 * c + 40]
        h = jnp.where(inside, value, 0.0).astype(BF16).astype(F32)
        moved = [jnp.take_along_axis(h[8 * g : 8 * g + 8], index[8 * g : 8 * g + 8], axis=1) for g in range(5)]
        applied_rows.append(jnp.where(ent >= 0, jnp.concatenate(moved, axis=0), 0.0))
        masked.append(jnp.where(ent >= 0, orb_ref[c].astype(F32), 0.0))
        out_ref[c] = applied_rows[c].astype(BF16)
    message = jnp.concatenate(masked + applied_rows, axis=0).astype(BF16)
    for y in range(8):
        msg_ref[y] = message


def rows_kernel(psi_ref, p_ref, psi_s):
    for c in range(2):
        for k, z in enumerate(Z_ORDER):
            at = (2 * z + c) * 80
            for part in range(2):
                psi_s[at + 40 * part : at + 40 * part + 40, :] = psi_ref[c, k, part].astype(F32)
    pad = jnp.zeros((8, 128), F32)
    for part in range(2):
        for s in range(40):
            block = jnp.concatenate([psi_s[pl.ds(40 * part + s, 24, stride=80), :], pad], axis=0)
            p_ref[part, :, 128 * s : 128 * s + 128] = block.astype(BF16)


def product_kernel(p_ref, own_ref, block_ref, own_s):
    for k, y in enumerate(Y_ORDER):
        own_s[160 * y : 160 * y + 160, :] = own_ref[k].astype(F32)

    def entries(first):
        rows = [own_s[pl.ds(first + s, 8, stride=160), :] for s in range(40)]
        return jnp.concatenate(rows, axis=1)

    m_re, m_im, a_re, a_im = [entries(40 * q) for q in range(4)]
    left_re = jnp.concatenate([m_re, m_im, a_re, a_im], axis=0).astype(BF16)
    left_im = jnp.concatenate([m_im, -m_re, a_im, -a_re], axis=0).astype(BF16)
    block = (mm_nt(left_re, p_ref[0]) + mm_nt(left_im, p_ref[1])) * (1.0 / 16384.0)
    shift = (128 - 2 * lax.axis_index("z")) % 128
    corr = block[:16, :24]
    corr = pltpu.roll(jnp.concatenate([corr, corr, jnp.zeros((16, 80), F32)], axis=1), shift, 1)
    row = [block[16:24, :24], block[24:, :24], corr[:8, :14], corr[8:, :14], jnp.zeros((8, 52), F32)]
    row = jnp.concatenate(row, axis=1)
    for peer in range(32):
        block_ref[peer] = row


def join_kernel(blocks_ref, joined_ref):
    def part(y, x):
        return blocks_ref[YX_ORDER.index(4 * y + x)]

    sums = [(part(y, 0) + part(y, 1)) + (part(y, 2) + part(y, 3)) for y in range(8)]
    ham = [jnp.concatenate([sums[y][:, 24 * m : 24 * m + 24] for y in range(8)], axis=1) for m in range(2)]
    pad = [jnp.zeros((8, 16), F32)]
    corr = [
        jnp.concatenate([sums[y][:, 48 + 14 * m : 62 + 14 * m] for y in range(8)] + pad, axis=1) for m in range(2)
    ]
    tail = jnp.concatenate([ham[0][:, 128:], ham[1][:, 128:]], axis=1)
    joined = jnp.concatenate([ham[0][:, :128], ham[1][:, :128], tail] + corr, axis=0)
    for z in range(12):
        joined_ref[z] = joined


def corr_lanes():
    lane = np.arange(256)
    ahead = (lane % 24 - 2 * np.arange(12)[:, None]) % 24
    source = np.where((ahead < 14) & (lane < 192), lane // 24 * 14 + ahead, 0)
    return source.reshape(24, 128).astype(np.int32)


def last_kernel(all_ref, lane_ref, s_hbm, h_hbm, t_s, out_s, sems):
    for c in range(2):
        for k, z in enumerate(TAIL_ORDER):
            rows = pl.ds(z * 2 + c, 8, stride=24)
            tail = all_ref[c, k, 16:24, :]
            t_s[0, rows, :] = all_ref[c, k, 0:8, :]
            t_s[1, rows, :] = tail
            t_s[2, rows, :] = all_ref[c, k, 8:16, :]
            t_s[3, rows, :] = jnp.concatenate([tail[:, 64:], tail[:, :64]], axis=1)
    sends = []
    for m in range(2):
        out_s[m, 0:128, :] = t_s[2 * m].T
        out_s[m, 128:192, :] = t_s[2 * m + 1].T[:64]
        sends.append(pltpu.make_async_copy(out_s.at[m], h_hbm.at[m], sems.at[m]))
        sends[-1].start()
    for k, z in enumerate(TAIL_ORDER):
        low = jnp.broadcast_to(lane_ref[2 * z : 2 * z + 1, :], (8, 128))
        high = jnp.broadcast_to(lane_ref[2 * z + 1 : 2 * z + 2, :], (8, 128))
        for c in range(2):
            rows = pl.ds(z * 2 + c, 8, stride=24)
            for m in range(2):
                corr = all_ref[c, k, 24 + 8 * m : 32 + 8 * m, :]
                t_s[4 + 2 * m, rows, :] = jnp.take_along_axis(corr, low, axis=1)
                t_s[5 + 2 * m, rows, :] = jnp.take_along_axis(corr, high, axis=1)

    def z_of(band):
        return (band >> 1) - 12 * ((band * 2731) >> 16)

    for m in range(2):
        low, high = t_s[4 + 2 * m], t_s[5 + 2 * m]
        for start, count, turned in ((0, 128, low.T), (128, 64, high.T[:64])):
            band_i = lax.broadcasted_iota(jnp.int32, (count, 192), 0) + start
            band_j = lax.broadcasted_iota(jnp.int32, (count, 192), 1)
            ahead = z_of(band_i) - z_of(band_j)
            direct = ((ahead >= 0) & (ahead <= 6)) | (ahead <= -6)
            mirror = jnp.concatenate([low[start : start + count], high[start : start + count, :64]], axis=1)
            out_s[2 + m, start : start + count, :] = jnp.where(direct, turned, mirror if m == 0 else -mirror)
        sends.append(pltpu.make_async_copy(out_s.at[2 + m], s_hbm.at[m], sems.at[2 + m]))
        sends[-1].start()
    for send in sends:
        send.wait()


def call(kernel, outs, *args, scratch=(), **space):
    return pl.pallas_call(
        kernel,
        out_shape=outs,
        scratch_shapes=list(scratch),
        compiler_params=pltpu.CompilerParams(vmem_limit_bytes=48 * 1024 * 1024),
        **space,
    )(*args)


def shape(dims, dtype):
    return jax.ShapeDtypeStruct(dims, dtype)


def exchange(array, axis, order):
    return lax.all_to_all(array, axis, 0, 0, tiled=True, axis_index_groups=[order])


def body(orbitals, potential, slot_sticks, stick_entries):
    wz, wx, bx, bz = tables(potential.shape[1], 64)
    args = [stick_entries, orbitals.reshape(2, 40, 128), potential, slot_sticks.reshape(1, 160)]
    zmsg, ent, own, pot, slots = call(
        start_kernel,
        [
            shape((12, 2, 40, 128), BF16),
            shape((40, 128), jnp.int32),
            shape((2, 40, 128), BF16),
            shape((120, 480), F32),
            shape((1, 160), jnp.int32),
        ],
        *[pltpu.with_memory_space_constraint(a, pltpu.HBM) for a in args],
        scratch=[pltpu.SemaphoreType.DMA((16,))],
        in_specs=[pl.BlockSpec(memory_space=pltpu.HBM)] * 4,
        out_specs=[pl.BlockSpec(memory_space=pltpu.HBM)] + [pl.BlockSpec(memory_space=pltpu.VMEM)] * 4,
    )
    psi = exchange(zmsg, "z", Z_ORDER)
    packed = call(first_kernel, shape((560, 128), BF16), ent, own, pot, bx)
    everyone = lax.all_gather(packed, "x")
    msg, out = call(
        main_kernel,
        [shape((8, 160, 128), BF16), shape((2, 40, 128), BF16)],
        everyone, own, ent, slots, slots.reshape(160, 1), wz, wx, bz,
    )
    arrived = exchange(msg, "y", Y_ORDER)
    rows = call(
        rows_kernel, shape((2, 32, 5120), BF16), lax.all_gather(psi, "c"), scratch=[pltpu.VMEM((1920, 128), F32)]
    )
    block = call(product_kernel, shape((32, 8, 128), F32), rows, arrived, scratch=[pltpu.VMEM((1280, 128), F32)])
    blocks = exchange(block, ("y", "x"), YX_ORDER)
    joined = call(join_kernel, shape((12, 40, 128), F32), blocks)
    joined = exchange(joined, "z", TAIL_ORDER)
    correlation, reduced = call(
        last_kernel,
        [shape((2, 192, 192), F32), shape((2, 192, 192), F32)],
        lax.all_gather(joined, "c"), corr_lanes(),
        scratch=[pltpu.VMEM((8, 192, 128), F32), pltpu.VMEM((4, 192, 192), F32), pltpu.SemaphoreType.DMA((4,))],
        out_specs=[pl.BlockSpec(memory_space=pltpu.HBM)] * 2,
    )
    return out.reshape(orbitals.shape), correlation, reduced


def solution(mesh):
    finer = Mesh(mesh.devices.reshape(8, 12, 2, mesh.shape["ga"]), ("y", "z", "c", "x"))
    return jax.shard_map(
        body,
        mesh=finer,
        in_specs=(P(None, BAND, "x", None), P("x", None), P(), P()),
        out_specs=(P(None, BAND, "x", None), P(), P()),
        check_vma=False,
    )
```

```python
import functools

import jax
import jax.numpy as jnp
import numpy as np
from jax import lax
from jax.experimental import pallas as pl
from jax.experimental.pallas import tpu as pltpu
from jax.sharding import Mesh
from jax.sharding import PartitionSpec as P

BAND = ("y", "z", "c")
M = 256
F32 = jnp.float32
BF16 = jnp.bfloat16

FIRST_Z, FIRST_Y, FIRST_YX, LAST_Z = 11, 3, (3, 2), 5


def turned(first, count):
    return [(first + k) % count for k in range(count)]


def outward(first, count):
    return [(first + (k + 1) // 2 * (1 if k % 2 else -1)) % count for k in range(count)]


Z_ORDER, Y_ORDER, TAIL_ORDER = turned(FIRST_Z, 12), outward(FIRST_Y, 8), outward(LAST_Z, 12)
YX_ORDER = [4 * y + x for y in turned(FIRST_YX[0], 8) for x in turned(FIRST_YX[1], 4)]


def hi_lo(table):
    hi = table.astype(np.float32).astype(jnp.bfloat16)
    lo = (table - hi.astype(np.float64)).astype(np.float32).astype(jnp.bfloat16)
    return np.stack([hi, lo])


def tables(points, radius):
    freq = np.arange(2 * radius) - radius + 1
    pos = np.arange(M)
    ang = 2.0 * np.pi * ((freq[:, None] * pos[None, :]) % M) / M
    cos, sin = np.cos(ang), np.sin(ang)
    wz = np.block([[cos, sin], [-sin, cos]])
    top = 2 * radius - 2
    q = np.arange(1, top + 1)
    shift = pos[:, None] / M - np.arange(points)[None, :] / points
    resample = np.ones((M, points))
    for k in q:
        resample += 2.0 * np.cos(2.0 * np.pi * k * shift)
    resample /= points
    return hi_lo(wz), hi_lo(wz.T), hi_lo(resample.T), hi_lo(resample)


def split(x):
    hi = x.astype(BF16)
    return hi, (x - hi.astype(F32)).astype(BF16)


def mm(a, b):
    return lax.dot_general(a, b, (((1,), (0,)), ((), ())), preferred_element_type=F32)


def mm_nt(a, b):
    return lax.dot_general(a, b, (((1,), (1,)), ((), ())), preferred_element_type=F32)


def start_kernel(
    ent_hbm, orb_hbm, pot_hbm, slot_hbm, zmsg_hbm, ent_ref, orb_ref, pot_ref, slot_ref, sems
):
    first = pl.multiple_of(lax.axis_index("x") * 40, 8)
    pairs = [(orb_hbm, orb_ref), (ent_hbm.at[pl.ds(first, 40), :], ent_ref), (pot_hbm, pot_ref)]
    pairs.append((slot_hbm, slot_ref))
    pairs += [(orb_ref, zmsg_hbm.at[z]) for z in range(12)]
    copies = [pltpu.make_async_copy(src, dst, sems.at[i]) for i, (src, dst) in enumerate(pairs)]
    for copy in copies[:4]:
        copy.start()
    copies[0].wait()
    for copy in copies[4:]:
        copy.start()
    for copy in copies[1:]:
        copy.wait()


def first_kernel(ent_ref, orb_ref, pot_ref, bx_ref, packed_ref):
    ent_t = ent_ref[...].T
    orb = orb_ref[...].astype(F32)
    lane = lax.broadcasted_iota(jnp.int32, (128, 128), 1)
    sub = lax.broadcasted_iota(jnp.int32, (128, 128), 0)
    pieces = [[], []]
    for g in range(5):
        rows = []
        for r in range(8):
            s = 8 * g + r
            match = ent_t[:, s : s + 1] == lane
            rows.append(jnp.max(jnp.where(match, sub, -1), axis=0, keepdims=True))
        source = jnp.concatenate(rows, axis=0)
        index = jnp.maximum(source, 0)
        for c in range(2):
            moved = jnp.take_along_axis(orb[c, 8 * g : 8 * g + 8, :], index, axis=1)
            pieces[c].append(jnp.where(source >= 0, moved, 0.0))
    spread = jnp.concatenate(pieces[0] + pieces[1], axis=0).astype(BF16)
    packed_ref[0:80, :] = spread
    v_hi, v_lo = split(pot_ref[...])
    vx = mm(v_hi, bx_ref[0]) + mm(v_lo, bx_ref[0]) + mm(v_hi, bx_ref[1])
    vx = jnp.concatenate([vx[:, :128], vx[:, 128:]], axis=0)
    hi, lo = split(vx)
    packed_ref[80:320, :] = hi
    packed_ref[320:560, :] = lo


def main_kernel(all_ref, orb_ref, ent_ref, slot_row_ref, slot_col_ref, wz_ref, wx_ref, bz_ref, msg_hbm, out_ref, msg_s, *sems):
    d = lax.axis_index("x")
    first = pl.multiple_of(d * 40, 8)

    ent = ent_ref[...]
    for c in range(2):
        msg_s[40 * c : 40 * c + 40, :] = jnp.where(ent >= 0, orb_ref[c].astype(F32), 0.0)
    msg_t = msg_s[...].astype(BF16)
    half_s = sems[0]
    half_s[0] = msg_t
    sends = []

    def send(part):
        for y in range(8):
            target = msg_hbm.at[y, pl.ds(80 * part, 80), :]
            sends.append(pltpu.make_async_copy(half_s.at[part], target, sems[1].at[8 * part + y]))
            sends[-1].start()

    send(0)

    def rows_of_all(start, count):
        return jnp.concatenate([all_ref[k, start : start + count, :].astype(F32) for k in range(4)], axis=0)

    def gathered_v(start):
        halves = [rows_of_all(start, 120), rows_of_all(start + 120, 120)]
        return jnp.concatenate(halves, axis=1).astype(BF16)

    v_hi = gathered_v(80)
    v_lo = gathered_v(320)
    pot = mm(bz_ref[0], v_hi) + mm(bz_ref[1], v_hi) + mm(bz_ref[0], v_lo)
    pot = pot.T

    place = (
        lax.broadcasted_iota(jnp.int32, (128, 160), 0) == jnp.broadcast_to(slot_row_ref[...], (128, 160))
    ).astype(F32).astype(BF16)
    c_re = rows_of_all(0, 40).astype(BF16)
    c_im = rows_of_all(40, 40).astype(BF16)
    sticks = jnp.concatenate([mm(place, c_re), mm(place, c_im)], axis=0).astype(BF16)

    t = mm(wx_ref[0], sticks) + mm(wx_ref[1], sticks)
    t = jnp.concatenate([t[:M], t[M:]], axis=1)
    t_hi, t_lo = split(t)
    field = mm(t_hi, wz_ref[0]) + mm(t_lo, wz_ref[0]) + mm(t_hi, wz_ref[1])
    prod = jnp.concatenate([field[:, :M] * pot, field[:, M:] * pot], axis=1)
    p_hi, p_lo = split(prod)
    y = mm(p_hi, wx_ref[0]) + mm(p_lo, wx_ref[0]) + mm(p_hi, wx_ref[1])
    y = jnp.concatenate([y[:, :128], y[:, 128:]], axis=0)
    y_hi, y_lo = split(y)

    slot = slot_col_ref[pl.ds(first, 40), :]
    pick = (lax.broadcasted_iota(jnp.int32, (40, 128), 1) == slot).astype(F32)
    none = jnp.zeros((40, 128), F32)
    pick = jnp.concatenate(
        [jnp.concatenate([pick, none], axis=1), jnp.concatenate([none, pick], axis=1)], axis=0
    ).astype(BF16)
    w_hi = mm(pick, wz_ref[0]).astype(BF16)
    w_lo = mm(pick, wz_ref[1]).astype(BF16)
    applied = (mm(w_hi, y_hi) + mm(w_hi, y_lo) + mm(w_lo, y_hi)) * (1.0 / (M * M))

    gx = slot - 63
    gz = lax.broadcasted_iota(jnp.int32, (40, 128), 1) - 63
    square = gx * gx + gz * gz
    inside = (square < 64 * 64) & (slot >= 0)
    kinetic = square.astype(F32) * (1.0 / 4096.0)
    own = all_ref[d, 0:80, :].astype(F32)
    index = jnp.maximum(ent, 0)
    applied_rows = []
    for c in range(2):
        value = kinetic * own[40 * c : 40 * c + 40] + applied[40 * c : 40 * c + 40]
        h = jnp.where(inside, value, 0.0).astype(BF16).astype(F32)
        moved = [jnp.take_along_axis(h[8 * g : 8 * g + 8], index[8 * g : 8 * g + 8], axis=1) for g in range(5)]
        applied_rows.append(jnp.where(ent >= 0, jnp.concatenate(moved, axis=0), 0.0))
        out_ref[c] = applied_rows[c].astype(BF16)
    half_s[1] = jnp.concatenate(applied_rows, axis=0).astype(BF16)
    send(1)
    for copy in sends:
        copy.wait()


def rows_kernel(psi_ref, p_ref, psi_s):
    for c in range(2):
        for k, z in enumerate(Z_ORDER):
            at = (2 * z + c) * 80
            for part in range(2):
                psi_s[at + 40 * part : at + 40 * part + 40, :] = psi_ref[c, k, part].astype(F32)
    pad = jnp.zeros((8, 128), F32)
    for part in range(2):
        for s in range(40):
            block = jnp.concatenate([psi_s[pl.ds(40 * part + s, 24, stride=80), :], pad], axis=0)
            p_ref[part, :, 128 * s : 128 * s + 128] = block.astype(BF16)


def product_kernel(p_ref, own_ref, block_ref, own_s):
    for k, y in enumerate(Y_ORDER):
        own_s[160 * y : 160 * y + 160, :] = own_ref[k].astype(F32)

    def entries(first):
        rows = [own_s[pl.ds(first + s, 8, stride=160), :] for s in range(40)]
        return jnp.concatenate(rows, axis=1)

    m_re, m_im, a_re, a_im = [entries(40 * q) for q in range(4)]
    left_re = jnp.concatenate([m_re, m_im, a_re, a_im], axis=0).astype(BF16)
    left_im = jnp.concatenate([m_im, -m_re, a_im, -a_re], axis=0).astype(BF16)
    block = (mm_nt(left_re, p_ref[0]) + mm_nt(left_im, p_ref[1])) * (1.0 / 16384.0)
    shift = (128 - 2 * lax.axis_index("z")) % 128
    corr = block[:16, :24]
    corr = pltpu.roll(jnp.concatenate([corr, corr, jnp.zeros((16, 80), F32)], axis=1), shift, 1)
    row = [block[16:24, :24], block[24:, :24], corr[:8, :14], corr[8:, :14], jnp.zeros((8, 52), F32)]
    row = jnp.concatenate(row, axis=1)
    for peer in range(32):
        block_ref[peer] = row


def join_kernel(blocks_ref, joined_ref):
    def part(y, x):
        return blocks_ref[YX_ORDER.index(4 * y + x)]

    sums = [(part(y, 0) + part(y, 1)) + (part(y, 2) + part(y, 3)) for y in range(8)]
    ham = [jnp.concatenate([sums[y][:, 24 * m : 24 * m + 24] for y in range(8)], axis=1) for m in range(2)]
    pad = [jnp.zeros((8, 16), F32)]
    corr = [
        jnp.concatenate([sums[y][:, 48 + 14 * m : 62 + 14 * m] for y in range(8)] + pad, axis=1) for m in range(2)
    ]
    tail = jnp.concatenate([ham[0][:, 128:], ham[1][:, 128:]], axis=1)
    joined = jnp.concatenate([ham[0][:, :128], ham[1][:, :128], tail] + corr, axis=0)
    for z in range(12):
        joined_ref[z] = joined


def corr_lanes():
    lane = np.arange(256)
    ahead = (lane % 24 - 2 * np.arange(12)[:, None]) % 24
    source = np.where((ahead < 14) & (lane < 192), lane // 24 * 14 + ahead, 0)
    return source.reshape(24, 128).astype(np.int32)


def last_kernel(all_ref, lane_ref, s_hbm, h_hbm, t_s, out_s, sems):
    for c in range(2):
        for k, z in enumerate(TAIL_ORDER):
            rows = pl.ds(z * 2 + c, 8, stride=24)
            tail = all_ref[c, k, 16:24, :]
            t_s[0, rows, :] = all_ref[c, k, 0:8, :]
            t_s[1, rows, :] = tail
            t_s[2, rows, :] = all_ref[c, k, 8:16, :]
            t_s[3, rows, :] = jnp.concatenate([tail[:, 64:], tail[:, :64]], axis=1)
    sends = []
    for m in range(2):
        out_s[m, 0:128, :] = t_s[2 * m].T
        out_s[m, 128:192, :] = t_s[2 * m + 1].T[:64]
        sends.append(pltpu.make_async_copy(out_s.at[m], h_hbm.at[m], sems.at[m]))
        sends[-1].start()
    for k, z in enumerate(TAIL_ORDER):
        low = jnp.broadcast_to(lane_ref[2 * z : 2 * z + 1, :], (8, 128))
        high = jnp.broadcast_to(lane_ref[2 * z + 1 : 2 * z + 2, :], (8, 128))
        for c in range(2):
            rows = pl.ds(z * 2 + c, 8, stride=24)
            for m in range(2):
                corr = all_ref[c, k, 24 + 8 * m : 32 + 8 * m, :]
                t_s[4 + 2 * m, rows, :] = jnp.take_along_axis(corr, low, axis=1)
                t_s[5 + 2 * m, rows, :] = jnp.take_along_axis(corr, high, axis=1)

    def z_of(band):
        return (band >> 1) - 12 * ((band * 2731) >> 16)

    for m in range(2):
        low, high = t_s[4 + 2 * m], t_s[5 + 2 * m]
        for start, count, turned in ((0, 128, low.T), (128, 64, high.T[:64])):
            band_i = lax.broadcasted_iota(jnp.int32, (count, 192), 0) + start
            band_j = lax.broadcasted_iota(jnp.int32, (count, 192), 1)
            ahead = z_of(band_i) - z_of(band_j)
            direct = ((ahead >= 0) & (ahead <= 6)) | (ahead <= -6)
            mirror = jnp.concatenate([low[start : start + count], high[start : start + count, :64]], axis=1)
            out_s[2 + m, start : start + count, :] = jnp.where(direct, turned, mirror if m == 0 else -mirror)
        sends.append(pltpu.make_async_copy(out_s.at[2 + m], s_hbm.at[m], sems.at[2 + m]))
        sends[-1].start()
    for send in sends:
        send.wait()


def call(kernel, outs, *args, scratch=(), **space):
    return pl.pallas_call(
        kernel,
        out_shape=outs,
        scratch_shapes=list(scratch),
        compiler_params=pltpu.CompilerParams(vmem_limit_bytes=48 * 1024 * 1024),
        **space,
    )(*args)


def shape(dims, dtype):
    return jax.ShapeDtypeStruct(dims, dtype)


def exchange(array, axis, order):
    return lax.all_to_all(array, axis, 0, 0, tiled=True, axis_index_groups=[order])


def body(orbitals, potential, slot_sticks, stick_entries):
    wz, wx, bx, bz = tables(potential.shape[1], 64)
    args = [stick_entries, orbitals.reshape(2, 40, 128), potential, slot_sticks.reshape(1, 160)]
    zmsg, ent, own, pot, slots = call(
        start_kernel,
        [
            shape((12, 2, 40, 128), BF16),
            shape((40, 128), jnp.int32),
            shape((2, 40, 128), BF16),
            shape((120, 480), F32),
            shape((1, 160), jnp.int32),
        ],
        *[pltpu.with_memory_space_constraint(a, pltpu.HBM) for a in args],
        scratch=[pltpu.SemaphoreType.DMA((16,))],
        in_specs=[pl.BlockSpec(memory_space=pltpu.HBM)] * 4,
        out_specs=[pl.BlockSpec(memory_space=pltpu.HBM)] + [pl.BlockSpec(memory_space=pltpu.VMEM)] * 4,
    )
    psi = exchange(zmsg, "z", Z_ORDER)
    packed = call(first_kernel, shape((560, 128), BF16), ent, own, pot, bx)
    everyone = lax.all_gather(packed, "x")
    msg, out = call(
        main_kernel,
        [shape((8, 160, 128), BF16), shape((2, 40, 128), BF16)],
        everyone, own, ent, slots, slots.reshape(160, 1), wz, wx, bz,
        scratch=[pltpu.VMEM((80, 128), F32), pltpu.VMEM((2, 80, 128), BF16), pltpu.SemaphoreType.DMA((16,))],
        out_specs=[pl.BlockSpec(memory_space=pltpu.HBM), pl.BlockSpec(memory_space=pltpu.VMEM)],
    )
    arrived = exchange(msg, "y", Y_ORDER)
    rows = call(
        rows_kernel, shape((2, 32, 5120), BF16), lax.all_gather(psi, "c"), scratch=[pltpu.VMEM((1920, 128), F32)]
    )
    block = call(product_kernel, shape((32, 8, 128), F32), rows, arrived, scratch=[pltpu.VMEM((1280, 128), F32)])
    blocks = exchange(block, ("y", "x"), YX_ORDER)
    joined = call(join_kernel, shape((12, 40, 128), F32), blocks)
    joined = exchange(joined, "z", TAIL_ORDER)
    correlation, reduced = call(
        last_kernel,
        [shape((2, 192, 192), F32), shape((2, 192, 192), F32)],
        lax.all_gather(joined, "c"), corr_lanes(),
        scratch=[pltpu.VMEM((8, 192, 128), F32), pltpu.VMEM((4, 192, 192), F32), pltpu.SemaphoreType.DMA((4,))],
        out_specs=[pl.BlockSpec(memory_space=pltpu.HBM)] * 2,
    )
    return out.reshape(orbitals.shape), correlation, reduced


def solution(mesh):
    finer = Mesh(mesh.devices.reshape(8, 12, 2, mesh.shape["ga"]), ("y", "z", "c", "x"))
    return jax.shard_map(
        body,
        mesh=finer,
        in_specs=(P(None, BAND, "x", None), P("x", None), P(), P()),
        out_specs=(P(None, BAND, "x", None), P(), P()),
        check_vma=False,
    )
```

```python
import functools

import jax
import jax.numpy as jnp
import numpy as np
from jax import lax
from jax.experimental import pallas as pl
from jax.experimental.pallas import tpu as pltpu
from jax.sharding import Mesh
from jax.sharding import PartitionSpec as P

BAND = ("y", "z", "c")
M = 256
F32 = jnp.float32
BF16 = jnp.bfloat16

FIRST_Z, FIRST_Y, FIRST_YX, LAST_Z = 11, 3, (3, 2), 5


def turned(first, count):
    return [(first + k) % count for k in range(count)]


def outward(first, count):
    return [(first + (k + 1) // 2 * (1 if k % 2 else -1)) % count for k in range(count)]


Z_ORDER, Y_ORDER, TAIL_ORDER = turned(FIRST_Z, 12), outward(FIRST_Y, 8), outward(LAST_Z, 12)
YX_ORDER = [4 * y + x for y in outward(FIRST_YX[0], 8) for x in outward(FIRST_YX[1], 4)]


def hi_lo(table):
    hi = table.astype(np.float32).astype(jnp.bfloat16)
    lo = (table - hi.astype(np.float64)).astype(np.float32).astype(jnp.bfloat16)
    return np.stack([hi, lo])


def tables(points, radius):
    freq = np.arange(2 * radius) - radius + 1
    pos = np.arange(M)
    ang = 2.0 * np.pi * ((freq[:, None] * pos[None, :]) % M) / M
    cos, sin = np.cos(ang), np.sin(ang)
    wz = np.block([[cos, sin], [-sin, cos]])
    top = 2 * radius - 2
    q = np.arange(1, top + 1)
    shift = pos[:, None] / M - np.arange(points)[None, :] / points
    resample = np.ones((M, points))
    for k in q:
        resample += 2.0 * np.cos(2.0 * np.pi * k * shift)
    resample /= points
    return hi_lo(wz), hi_lo(wz.T), hi_lo(resample.T), hi_lo(resample)


def split(x):
    hi = x.astype(BF16)
    return hi, (x - hi.astype(F32)).astype(BF16)


def mm(a, b):
    return lax.dot_general(a, b, (((1,), (0,)), ((), ())), preferred_element_type=F32)


def mm_nt(a, b):
    return lax.dot_general(a, b, (((1,), (1,)), ((), ())), preferred_element_type=F32)


def start_kernel(
    ent_hbm, orb_hbm, pot_hbm, slot_hbm, zmsg_hbm, ent_ref, orb_ref, pot_ref, slot_ref, sems
):
    first = pl.multiple_of(lax.axis_index("x") * 40, 8)
    pairs = [(orb_hbm, orb_ref), (ent_hbm.at[pl.ds(first, 40), :], ent_ref), (pot_hbm, pot_ref)]
    pairs.append((slot_hbm, slot_ref))
    pairs += [(orb_ref, zmsg_hbm.at[z]) for z in range(12)]
    copies = [pltpu.make_async_copy(src, dst, sems.at[i]) for i, (src, dst) in enumerate(pairs)]
    for copy in copies[:4]:
        copy.start()
    copies[0].wait()
    for copy in copies[4:]:
        copy.start()
    for copy in copies[1:]:
        copy.wait()


def first_kernel(ent_ref, orb_ref, pot_ref, bx_ref, packed_ref):
    ent_t = ent_ref[...].T
    orb = orb_ref[...].astype(F32)
    lane = lax.broadcasted_iota(jnp.int32, (128, 128), 1)
    sub = lax.broadcasted_iota(jnp.int32, (128, 128), 0)
    pieces = [[], []]
    for g in range(5):
        rows = []
        for r in range(8):
            s = 8 * g + r
            match = ent_t[:, s : s + 1] == lane
            rows.append(jnp.max(jnp.where(match, sub, -1), axis=0, keepdims=True))
        source = jnp.concatenate(rows, axis=0)
        index = jnp.maximum(source, 0)
        for c in range(2):
            moved = jnp.take_along_axis(orb[c, 8 * g : 8 * g + 8, :], index, axis=1)
            pieces[c].append(jnp.where(source >= 0, moved, 0.0))
    spread = jnp.concatenate(pieces[0] + pieces[1], axis=0).astype(BF16)
    packed_ref[0:80, :] = spread
    v_hi, v_lo = split(pot_ref[...])
    vx = mm(v_hi, bx_ref[0]) + mm(v_lo, bx_ref[0]) + mm(v_hi, bx_ref[1])
    vx = jnp.concatenate([vx[:, :128], vx[:, 128:]], axis=0)
    hi, lo = split(vx)
    packed_ref[80:320, :] = hi
    packed_ref[320:560, :] = lo


def main_kernel(all_ref, orb_ref, ent_ref, slot_row_ref, slot_col_ref, wz_ref, wx_ref, bz_ref, msg_ref, out_ref):
    d = lax.axis_index("x")
    first = pl.multiple_of(d * 40, 8)

    def rows_of_all(start, count):
        return jnp.concatenate([all_ref[k, start : start + count, :].astype(F32) for k in range(4)], axis=0)

    def gathered_v(start):
        halves = [rows_of_all(start, 120), rows_of_all(start + 120, 120)]
        return jnp.concatenate(halves, axis=1).astype(BF16)

    v_hi = gathered_v(80)
    v_lo = gathered_v(320)
    pot = mm(bz_ref[0], v_hi) + mm(bz_ref[1], v_hi) + mm(bz_ref[0], v_lo)
    pot = pot.T

    place = (
        lax.broadcasted_iota(jnp.int32, (128, 160), 0) == jnp.broadcast_to(slot_row_ref[...], (128, 160))
    ).astype(F32).astype(BF16)
    c_re = rows_of_all(0, 40).astype(BF16)
    c_im = rows_of_all(40, 40).astype(BF16)
    sticks = jnp.concatenate([mm(place, c_re), mm(place, c_im)], axis=0).astype(BF16)

    t = mm(wx_ref[0], sticks) + mm(wx_ref[1], sticks)
    t = jnp.concatenate([t[:M], t[M:]], axis=1)
    t_hi, t_lo = split(t)
    field = mm(t_hi, wz_ref[0]) + mm(t_lo, wz_ref[0]) + mm(t_hi, wz_ref[1])
    prod = jnp.concatenate([field[:, :M] * pot, field[:, M:] * pot], axis=1)
    p_hi, p_lo = split(prod)
    y = mm(p_hi, wx_ref[0]) + mm(p_lo, wx_ref[0]) + mm(p_hi, wx_ref[1])
    y = jnp.concatenate([y[:, :128], y[:, 128:]], axis=0)
    y_hi, y_lo = split(y)

    slot = slot_col_ref[pl.ds(first, 40), :]
    pick = (lax.broadcasted_iota(jnp.int32, (40, 128), 1) == slot).astype(F32)
    none = jnp.zeros((40, 128), F32)
    pick = jnp.concatenate(
        [jnp.concatenate([pick, none], axis=1), jnp.concatenate([none, pick], axis=1)], axis=0
    ).astype(BF16)
    w_hi = mm(pick, wz_ref[0]).astype(BF16)
    w_lo = mm(pick, wz_ref[1]).astype(BF16)
    applied = (mm(w_hi, y_hi) + mm(w_hi, y_lo) + mm(w_lo, y_hi)) * (1.0 / (M * M))

    gx = slot - 63
    gz = lax.broadcasted_iota(jnp.int32, (40, 128), 1) - 63
    square = gx * gx + gz * gz
    inside = (square < 64 * 64) & (slot >= 0)
    kinetic = square.astype(F32) * (1.0 / 4096.0)
    own = all_ref[d, 0:80, :].astype(F32)
    ent = ent_ref[...]
    index = jnp.maximum(ent, 0)
    masked, applied_rows = [], []
    for c in range(2):
        value = kinetic * own[40 * c : 40 * c + 40] + applied[40 * c : 40 * c + 40]
        h = jnp.where(inside, value, 0.0).astype(BF16).astype(F32)
        moved = [jnp.take_along_axis(h[8 * g : 8 * g + 8], index[8 * g : 8 * g + 8], axis=1) for g in range(5)]
        applied_rows.append(jnp.where(ent >= 0, jnp.concatenate(moved, axis=0), 0.0))
        masked.append(jnp.where(ent >= 0, orb_ref[c].astype(F32), 0.0))
        out_ref[c] = applied_rows[c].astype(BF16)
    message = jnp.concatenate(masked + applied_rows, axis=0).astype(BF16)
    for y in range(8):
        msg_ref[y] = message


def rows_kernel(psi_ref, p_ref, psi_s):
    for c in range(2):
        for k, z in enumerate(Z_ORDER):
            at = (2 * z + c) * 80
            for part in range(2):
                psi_s[at + 40 * part : at + 40 * part + 40, :] = psi_ref[c, k, part].astype(F32)
    pad = jnp.zeros((8, 128), F32)
    for part in range(2):
        for s in range(40):
            block = jnp.concatenate([psi_s[pl.ds(40 * part + s, 24, stride=80), :], pad], axis=0)
            p_ref[part, :, 128 * s : 128 * s + 128] = block.astype(BF16)


def product_kernel(p_ref, own_ref, block_ref, own_s):
    for k, y in enumerate(Y_ORDER):
        own_s[160 * y : 160 * y + 160, :] = own_ref[k].astype(F32)

    def entries(first):
        rows = [own_s[pl.ds(first + s, 8, stride=160), :] for s in range(40)]
        return jnp.concatenate(rows, axis=1)

    m_re, m_im, a_re, a_im = [entries(40 * q) for q in range(4)]
    left_re = jnp.concatenate([m_re, m_im, a_re, a_im], axis=0).astype(BF16)
    left_im = jnp.concatenate([m_im, -m_re, a_im, -a_re], axis=0).astype(BF16)
    block = (mm_nt(left_re, p_ref[0]) + mm_nt(left_im, p_ref[1])) * (1.0 / 16384.0)
    shift = (128 - 2 * lax.axis_index("z")) % 128
    corr = block[:16, :24]
    corr = pltpu.roll(jnp.concatenate([corr, corr, jnp.zeros((16, 80), F32)], axis=1), shift, 1)
    row = [block[16:24, :24], block[24:, :24], corr[:8, :14], corr[8:, :14], jnp.zeros((8, 52), F32)]
    row = jnp.concatenate(row, axis=1)
    for peer in range(32):
        block_ref[peer] = row


def join_kernel(blocks_ref, joined_ref):
    def part(y, x):
        return blocks_ref[YX_ORDER.index(4 * y + x)]

    sums = [(part(y, 0) + part(y, 1)) + (part(y, 2) + part(y, 3)) for y in range(8)]
    ham = [jnp.concatenate([sums[y][:, 24 * m : 24 * m + 24] for y in range(8)], axis=1) for m in range(2)]
    pad = [jnp.zeros((8, 16), F32)]
    corr = [
        jnp.concatenate([sums[y][:, 48 + 14 * m : 62 + 14 * m] for y in range(8)] + pad, axis=1) for m in range(2)
    ]
    tail = jnp.concatenate([ham[0][:, 128:], ham[1][:, 128:]], axis=1)
    joined = jnp.concatenate([ham[0][:, :128], ham[1][:, :128], tail] + corr, axis=0)
    for z in range(12):
        joined_ref[z] = joined


def corr_lanes():
    lane = np.arange(256)
    ahead = (lane % 24 - 2 * np.arange(12)[:, None]) % 24
    source = np.where((ahead < 14) & (lane < 192), lane // 24 * 14 + ahead, 0)
    return source.reshape(24, 128).astype(np.int32)


def last_kernel(all_ref, lane_ref, s_hbm, h_hbm, t_s, out_s, sems):
    for c in range(2):
        for k, z in enumerate(TAIL_ORDER):
            rows = pl.ds(z * 2 + c, 8, stride=24)
            tail = all_ref[c, k, 16:24, :]
            t_s[0, rows, :] = all_ref[c, k, 0:8, :]
            t_s[1, rows, :] = tail
            t_s[2, rows, :] = all_ref[c, k, 8:16, :]
            t_s[3, rows, :] = jnp.concatenate([tail[:, 64:], tail[:, :64]], axis=1)
    sends = []
    for m in range(2):
        out_s[m, 0:128, :] = t_s[2 * m].T
        out_s[m, 128:192, :] = t_s[2 * m + 1].T[:64]
        sends.append(pltpu.make_async_copy(out_s.at[m], h_hbm.at[m], sems.at[m]))
        sends[-1].start()
    for k, z in enumerate(TAIL_ORDER):
        low = jnp.broadcast_to(lane_ref[2 * z : 2 * z + 1, :], (8, 128))
        high = jnp.broadcast_to(lane_ref[2 * z + 1 : 2 * z + 2, :], (8, 128))
        for c in range(2):
            rows = pl.ds(z * 2 + c, 8, stride=24)
            for m in range(2):
                corr = all_ref[c, k, 24 + 8 * m : 32 + 8 * m, :]
                t_s[4 + 2 * m, rows, :] = jnp.take_along_axis(corr, low, axis=1)
                t_s[5 + 2 * m, rows, :] = jnp.take_along_axis(corr, high, axis=1)

    def z_of(band):
        return (band >> 1) - 12 * ((band * 2731) >> 16)

    for m in range(2):
        low, high = t_s[4 + 2 * m], t_s[5 + 2 * m]
        for start, count, turned in ((0, 128, low.T), (128, 64, high.T[:64])):
            band_i = lax.broadcasted_iota(jnp.int32, (count, 192), 0) + start
            band_j = lax.broadcasted_iota(jnp.int32, (count, 192), 1)
            ahead = z_of(band_i) - z_of(band_j)
            direct = ((ahead >= 0) & (ahead <= 6)) | (ahead <= -6)
            mirror = jnp.concatenate([low[start : start + count], high[start : start + count, :64]], axis=1)
            out_s[2 + m, start : start + count, :] = jnp.where(direct, turned, mirror if m == 0 else -mirror)
        sends.append(pltpu.make_async_copy(out_s.at[2 + m], s_hbm.at[m], sems.at[2 + m]))
        sends[-1].start()
    for send in sends:
        send.wait()


def call(kernel, outs, *args, scratch=(), **space):
    return pl.pallas_call(
        kernel,
        out_shape=outs,
        scratch_shapes=list(scratch),
        compiler_params=pltpu.CompilerParams(vmem_limit_bytes=48 * 1024 * 1024),
        **space,
    )(*args)


def shape(dims, dtype):
    return jax.ShapeDtypeStruct(dims, dtype)


def exchange(array, axis, order):
    return lax.all_to_all(array, axis, 0, 0, tiled=True, axis_index_groups=[order])


def body(orbitals, potential, slot_sticks, stick_entries):
    wz, wx, bx, bz = tables(potential.shape[1], 64)
    args = [stick_entries, orbitals.reshape(2, 40, 128), potential, slot_sticks.reshape(1, 160)]
    zmsg, ent, own, pot, slots = call(
        start_kernel,
        [
            shape((12, 2, 40, 128), BF16),
            shape((40, 128), jnp.int32),
            shape((2, 40, 128), BF16),
            shape((120, 480), F32),
            shape((1, 160), jnp.int32),
        ],
        *[pltpu.with_memory_space_constraint(a, pltpu.HBM) for a in args],
        scratch=[pltpu.SemaphoreType.DMA((16,))],
        in_specs=[pl.BlockSpec(memory_space=pltpu.HBM)] * 4,
        out_specs=[pl.BlockSpec(memory_space=pltpu.HBM)] + [pl.BlockSpec(memory_space=pltpu.VMEM)] * 4,
    )
    psi = exchange(zmsg, "z", Z_ORDER)
    packed = call(first_kernel, shape((560, 128), BF16), ent, own, pot, bx)
    everyone = lax.all_gather(packed, "x")
    msg, out = call(
        main_kernel,
        [shape((8, 160, 128), BF16), shape((2, 40, 128), BF16)],
        everyone, own, ent, slots, slots.reshape(160, 1), wz, wx, bz,
    )
    arrived = exchange(msg, "y", Y_ORDER)
    rows = call(
        rows_kernel, shape((2, 32, 5120), BF16), lax.all_gather(psi, "c"), scratch=[pltpu.VMEM((1920, 128), F32)]
    )
    block = call(product_kernel, shape((32, 8, 128), F32), rows, arrived, scratch=[pltpu.VMEM((1280, 128), F32)])
    blocks = exchange(block, ("y", "x"), YX_ORDER)
    joined = call(join_kernel, shape((12, 40, 128), F32), blocks)
    joined = exchange(joined, "z", TAIL_ORDER)
    correlation, reduced = call(
        last_kernel,
        [shape((2, 192, 192), F32), shape((2, 192, 192), F32)],
        lax.all_gather(joined, "c"), corr_lanes(),
        scratch=[pltpu.VMEM((8, 192, 128), F32), pltpu.VMEM((4, 192, 192), F32), pltpu.SemaphoreType.DMA((4,))],
        out_specs=[pl.BlockSpec(memory_space=pltpu.HBM)] * 2,
    )
    return out.reshape(orbitals.shape), correlation, reduced


def solution(mesh):
    finer = Mesh(mesh.devices.reshape(8, 12, 2, mesh.shape["ga"]), ("y", "z", "c", "x"))
    return jax.shard_map(
        body,
        mesh=finer,
        in_specs=(P(None, BAND, "x", None), P("x", None), P(), P()),
        out_specs=(P(None, BAND, "x", None), P(), P()),
        check_vma=False,
    )
```
